32 devices in a mesh: dp: 16 (over z, x, core), fsdp: 2 (over y).
Axes of the slice: x: 2, y: 2, z: 4, core: 2. Of those that a mesh axis runs over, the one named last changes fastest.
Arguments:
- patches: bfloat16 [64, 1024, 768], P(('dp', 'fsdp')), may hold values from -6 to 6
- ln_gain: bfloat16 [2, 768], P(None, 'fsdp'), may hold values from 0.25 to 1.75
- ln_bias: bfloat16 [2, 768], P(None, 'fsdp'), may hold values from -1.5 to 1.5
- w_qkv: bfloat16 [768, 2304], P('fsdp'), may hold values from -0.21875 to 0.21875
- b_qkv: bfloat16 [2304], P('fsdp'), may hold values from -1.5 to 1.5
- qk_gain: bfloat16 [2, 64], P(None, 'fsdp'), may hold values from 0.25 to 1.75
- w_proj: bfloat16 [768, 768], P('fsdp'), may hold values from -1.75 to 1.75
- out_bias: bfloat16 [2, 768], P(None, 'fsdp'), may hold values from -1.5 to 1.5
- w_in: bfloat16 [768, 3072], P('fsdp'), may hold values from -0.21875 to 0.21875
- b_in: bfloat16 [3072], P('fsdp'), may hold values from -1.5 to 1.5
- w_out: bfloat16 [3072, 768], P('fsdp'), may hold values from -0.109375 to 0.109375
- lengths: int32 [64, 10], P(('dp', 'fsdp')), may hold values from 0 to 1024, as said below
- cotangent: bfloat16 [64, 1024, 768], P(('dp', 'fsdp')), may hold values from -6 to 6
Outputs:
- block_out: bfloat16 [64, 1024, 768], P(('dp', 'fsdp'))
- grad_patches: float32 [64, 1024, 768], P(('dp', 'fsdp'))
- grad_ln_gain: float32 [2, 768], P(None, 'fsdp')
- grad_ln_bias: float32 [2, 768], P(None, 'fsdp')
- grad_w_qkv: float32 [768, 2304], P('fsdp')
- grad_b_qkv: float32 [2304], P('fsdp')
- grad_qk_gain: float32 [2, 64], P(None, 'fsdp')
- grad_w_proj: float32 [768, 768], P('fsdp')
- grad_out_bias: float32 [2, 768], P(None, 'fsdp')
- grad_w_in: float32 [768, 3072], P('fsdp')
- grad_b_in: float32 [3072], P('fsdp')
- grad_w_out: float32 [3072, 768], P('fsdp')
The draws below stay inside these ranges and needn't reach their ends.
Inputs may be any that keep to these rules, and one draw needn't show every extreme that they name: In each row the nonzero lengths come first, each from 100 to 1024, and together they are at most 1024; the remaining entries are 0. The first row holds a single picture of 1024 patches.
All inputs are finite; a program needn't handle non-finite values.
Results may differ from the reference program's by a relative error of at most 0.019.
Values may be sent and summed in bfloat16 or wider, within the bound.
A program may use at most 384 MiB of HBM per device.

```python
import math
import jax
import jax.numpy as jnp
from jax import lax

D = 768
H = 12
FF = 3072
HD = 64
ROW = 1024
SHORTEST = 100
PICS = 10
ROWS = 64


def draw_lengths(key, part):
    drawn_len = jax.random.randint(key, (ROWS, PICS), SHORTEST, ROW + 1, dtype=jnp.int32)
    row_index = lax.broadcasted_iota(jnp.int32, (ROWS, PICS), 0)
    col_index = lax.broadcasted_iota(jnp.int32, (ROWS, PICS), 1)
    drawn_len = jnp.where((row_index == 0) & (col_index == 0), ROW, drawn_len).astype(jnp.int32)
    running = jnp.cumsum(drawn_len, axis=1).astype(jnp.int32)
    return jnp.where(running <= ROW, drawn_len, 0).astype(jnp.int32)


def shard_levels(rng, shape, cuts, least, top_value):
    factor_of, own = 1.0, jax.random.fold_in(rng, 6)
    for axis_at, shards_of in cuts:
        draws = jnp.exp(jax.random.uniform(jax.random.fold_in(own, axis_at), (shards_of,), jnp.float32, least / len(cuts), top_value / len(cuts)))
        factor_of = factor_of * jnp.repeat(draws, shape[axis_at] // shards_of).reshape([-1 if axis == axis_at else 1 for axis in range(len(shape))])
    return factor_of


def gaussian(key, shape, deviation, reach, pieces=(), held_as=jnp.bfloat16):
    entries = jax.random.normal(key, shape, jnp.float32) * deviation
    if len(pieces) > 0:
        entries = shard_levels(key, shape, pieces, -0.22, 0.18) * entries
    return jnp.clip(entries, min=-reach, max=reach).astype(held_as)


def setup_inputs(seed: int = 0) -> dict:
    key_of = jax.random.split(jax.random.key(seed), 14)
    patches = gaussian(key_of[0], (ROWS, ROW, D), 1.0, 6.0, ((0, 32),))
    ln_gain = jnp.clip(1.0 + 0.15 * jax.random.normal(key_of[1], (2, D), jnp.float32), 0.25, 1.75).astype(jnp.bfloat16)
    ln_bias = gaussian(key_of[2], (2, D), 0.3, 1.5, ((1, 2),))
    w_qkv = gaussian(key_of[3], (D, 3 * D), D ** -0.5, 0.21875, ((0, 2),))
    b_qkv = gaussian(key_of[4], (3 * D,), 0.3, 1.5, ((0, 2),))
    qk_gain = jnp.clip(1.0 + 0.15 * jax.random.normal(key_of[5], (2, HD), jnp.float32), 0.25, 1.75).astype(jnp.bfloat16)
    w_proj = gaussian(key_of[6], (D, D), (D // 64) ** -0.5, 1.75, ((0, 2),))
    out_bias = gaussian(key_of[7], (2, D), 0.3, 1.5, ((1, 2),))
    w_in = gaussian(key_of[8], (D, FF), D ** -0.5, 0.21875, ((0, 2),))
    b_in = gaussian(key_of[9], (FF,), 0.3, 1.5, ((0, 2),))
    w_out = gaussian(key_of[10], (FF, D), FF ** -0.5, 0.109375, ((0, 2),))
    lengths = draw_lengths(jax.random.fold_in(key_of[13], 71), 0)
    cotangent = gaussian(key_of[12], (ROWS, ROW, D), 1.0, 6.0, ((0, 32),))
    return dict(patches=patches, ln_gain=ln_gain, ln_bias=ln_bias, w_qkv=w_qkv, b_qkv=b_qkv, qk_gain=qk_gain, w_proj=w_proj, out_bias=out_bias, w_in=w_in, b_in=b_in, w_out=w_out, lengths=lengths, cotangent=cotangent)


@jax.custom_vjp
def low(v):
    return lax.optimization_barrier(v.astype(jnp.bfloat16)).astype(jnp.float32)

@jax.custom_vjp
def low_back(v):
    return v

def low_keep(v):
    return (low(v), None)

def low_pass(kept, grad):
    return (grad,)

def back_keep(v):
    return (v, None)

def back_low(kept, grad):
    return (low(grad),)
low.defvjp(low_keep, low_pass)
low_back.defvjp(back_keep, back_low)

def normalize(values, gain, shift):
    average = lax.optimization_barrier(jnp.mean(values, axis=-1, keepdims=True))
    centered = values - average
    variance = lax.optimization_barrier(jnp.mean(centered * centered, axis=-1, keepdims=True))
    return centered * lax.rsqrt(variance + 1e-06) * gain + shift

def picture_ids(row_lengths):
    pic_ends = jnp.cumsum(row_lengths).astype(jnp.int32)
    positions = jnp.arange(ROW, dtype=jnp.int32)
    pic_id = lax.optimization_barrier(jnp.sum((positions[:, None] >= pic_ends[None, :]).astype(jnp.int32), axis=1)).astype(jnp.int32)
    inside = (positions < pic_ends[PICS - 1]).astype(jnp.float32)
    return (pic_id, inside)

def block_forward(source, parameters, pic_id):
    ln_gain, ln_bias, w_qkv, b_qkv, qk_gain, w_proj, out_bias, w_in, b_in, w_out = parameters
    highest = lax.Precision.HIGHEST
    head_dim = D // H
    normed1 = low(normalize(source, ln_gain[0], ln_bias[0]))
    proj = low_back(jnp.dot(normed1, w_qkv, precision=highest) + b_qkv).reshape(ROW, 3, H, head_dim)
    queries = low(normalize(proj[:, 0], qk_gain[0], 0.0))
    keys_low = low(normalize(proj[:, 1], qk_gain[1], 0.0))
    values_low = low(proj[:, 2])
    scores = low_back(jnp.einsum('qhd,khd->hqk', queries, keys_low, precision=highest)) * (1.0 / math.sqrt(head_dim))
    same_pic = pic_id[:, None] == pic_id[None, :]
    scores = jnp.where(same_pic[None], scores, -1e+30)
    row_max = lax.optimization_barrier(jnp.max(scores, axis=-1, keepdims=True))
    exp_scores = jnp.exp(scores - row_max)
    probs = exp_scores / lax.optimization_barrier(jnp.sum(exp_scores, axis=-1, keepdims=True))
    attn = jnp.einsum('hqk,khd->qhd', low(probs), values_low, precision=highest).reshape(ROW, D)
    attn = low(low_back(attn))
    resid = source + low_back(jnp.dot(attn, w_proj, precision=highest) + out_bias[0])
    normed2 = low(normalize(resid, ln_gain[1], ln_bias[1]))
    hidden = low_back(jnp.dot(normed2, w_in, precision=highest) + b_in)
    activated = low(jax.nn.gelu(hidden))
    return resid + low_back(jnp.dot(activated, w_out, precision=highest) + out_bias[1])

def reference(patches, ln_gain, ln_bias, w_qkv, b_qkv, qk_gain, w_proj, out_bias, w_in, b_in, w_out, lengths, cotangent):
    parameters = tuple((item.astype(jnp.float32) for item in (ln_gain, ln_bias, w_qkv, b_qkv, qk_gain, w_proj, out_bias, w_in, b_in, w_out)))

    def one_row(totals, row_data):
        row_patches, row_lengths, row_cot = row_data
        pic_id, inside = picture_ids(row_lengths)

        def forward_only(source, params_now):
            return block_forward(source, params_now, pic_id)
        result, pullback = jax.vjp(forward_only, row_patches.astype(jnp.float32), parameters)
        grad_source, grad_params = pullback(row_cot.astype(jnp.float32) * inside[:, None])
        totals = jax.tree.map(lambda first, second: first + second, totals, grad_params)
        return (totals, (result.astype(jnp.bfloat16), grad_source))
    zeros_init = tuple((jnp.zeros_like(item) for item in parameters))
    totals, (block_out, grad_patches) = lax.scan(one_row, zeros_init, (patches, lengths, cotangent))
    return (block_out, grad_patches, totals[0], totals[1], totals[2], totals[3], totals[4], totals[5], totals[6], totals[7], totals[8], totals[9])
```

```python
import functools
import math

import jax
import jax.numpy as jnp
from jax import lax
from jax.experimental import pallas as pl
from jax.experimental.pallas import tpu as pltpu
from jax.sharding import PartitionSpec as P

H = 12
HD = 64
PAIR = 2 * HD
GROUP = 3
BLK = 256
MASK = 256.0
LOG2E = math.log2(math.e)
f32 = jnp.float32
bf16 = jnp.bfloat16
NT = (((1,), (1,)), ((), ()))


def dot(a, b):
    return jnp.dot(a, b, preferred_element_type=f32)


def dot_nt(a, b):
    return lax.dot_general(a, b, NT, preferred_element_type=f32)


def lanes(rows):
    return lax.broadcasted_iota(jnp.int32, (rows, PAIR), 1)


def half_matrix(same, value):
    i = lax.broadcasted_iota(jnp.int32, (PAIR, PAIR), 0) // HD
    j = lax.broadcasted_iota(jnp.int32, (PAIR, PAIR), 1) // HD
    hit = (i == j) if same else (i != j)
    return jnp.where(hit, value, 0.0).astype(bf16)


def head_stats(raw, averager):
    mean = dot(raw, averager)
    centered = raw.astype(f32) - mean
    variance = dot((centered * centered).astype(bf16), averager)
    rstd = lax.rsqrt(variance + 1e-6)
    return centered * rstd, rstd


def split(v):
    high = v.astype(bf16)
    low = (v - high.astype(f32)).astype(bf16)
    return high, low


def query_extra(pic, lane):
    slot = lane % HD
    hot = jnp.where(slot == pic, MASK, 0.0)
    return jnp.where(slot == 11, -MASK, hot)


def key_extra(pic, lane):
    slot = lane % HD
    hot = jnp.where(slot == pic, 1.0, 0.0)
    return jnp.where(slot == 11, 1.0, jnp.where((slot == 12) | (slot == 13), -1.0, hot))


def forward_kernel(
    bounds, q_ref, k_ref, v_ref, pic_ref, gain_ref, out_ref, lse_ref, qa, ka, va, acc
):
    row = pl.program_id(0)
    slots = q_ref.shape[1]
    blocks = slots // BLK
    averager = half_matrix(True, 1.0 / HD)
    lane = lanes(BLK)
    low_half = lane < HD
    heads = 2 * GROUP

    def prepare(b, _):
        at = pl.ds(pl.multiple_of(b * BLK, BLK), BLK)
        pic = pic_ref[0, at, :]
        q_more = query_extra(pic, lane)
        k_more = key_extra(pic, lane)
        for p in range(GROUP):
            col = slice(p * PAIR, (p + 1) * PAIR)
            normed, _unused = head_stats(q_ref[0, at, col], averager)
            q = (normed * gain_ref[0:1, :]).astype(bf16).astype(f32) * 0.125
            normed, _unused = head_stats(k_ref[0, at, col], averager)
            k = normed * gain_ref[1:2, :]
            v = v_ref[0, at, col].astype(f32)
            qa[2 * p, at, :] = jnp.where(low_half, q, q_more).astype(bf16)
            qa[2 * p + 1, at, :] = jnp.where(low_half, q_more, q).astype(bf16)
            ka[2 * p, at, :] = jnp.where(low_half, k, k_more).astype(bf16)
            ka[2 * p + 1, at, :] = jnp.where(low_half, k_more, k).astype(bf16)
            va[2 * p, at, :] = jnp.where(low_half, v, 1.0).astype(bf16)
            va[2 * p + 1, at, :] = jnp.where(low_half, 1.0, v).astype(bf16)
        return 0

    lax.fori_loop(0, blocks, prepare, 0)

    def query_block(b, _):
        at = pl.ds(pl.multiple_of(b * BLK, BLK), BLK)
        acc[...] = jnp.zeros_like(acc)

        def key_block(kb, _):
            keys = pl.ds(pl.multiple_of(kb * BLK, BLK), BLK)
            for h in range(heads):
                scores = dot_nt(qa[h, at, :], ka[h, keys, :])
                probs = jnp.exp2(scores * LOG2E).astype(bf16)
                acc[h] += dot(probs, va[h, keys, :])
            return 0

        lax.fori_loop(bounds[row, 0, b], bounds[row, 1, b], key_block, 0)
        for p in range(GROUP):
            col = slice(p * PAIR, (p + 1) * PAIR)
            even, odd = acc[2 * p], acc[2 * p + 1]
            crossed = jnp.where(low_half, odd, even)
            total = pltpu.roll(crossed, HD, 1)
            out_ref[0, at, col] = (jnp.where(low_half, even, odd) / total).astype(bf16)
            lse_ref[0, at, col] = jnp.log(crossed)
        return 0

    lax.fori_loop(0, blocks, query_block, 0)


def backward_kernel(
    bounds,
    q_ref,
    k_ref,
    v_ref,
    o_ref,
    g_ref,
    lse_ref,
    pic_ref,
    gain_ref,
    out_ref,
    stat_ref,
    qa,
    ka,
    va,
    ga,
    kt,
    dqt,
    dk,
    dv,
):
    row = pl.program_id(0)
    slots = q_ref.shape[1]
    blocks = slots // BLK
    averager = half_matrix(True, 1.0 / HD)
    crosser = half_matrix(False, 1.0)
    lane = lanes(BLK)
    slot = lane % HD
    low_half = lane < HD
    heads = 2 * GROUP

    def prepare(b, _):
        at = pl.ds(pl.multiple_of(b * BLK, BLK), BLK)
        pic = pic_ref[0, at, :]
        q_hot = query_extra(pic, lane)
        k_more = key_extra(pic, lane)
        for p in range(GROUP):
            col = slice(p * PAIR, (p + 1) * PAIR)
            lse = lse_ref[0, at, col]
            lse_high = lse.astype(bf16).astype(f32)
            q_more = jnp.where(slot == 12, lse_high, jnp.where(slot == 13, lse - lse_high, q_hot))
            normed, _unused = head_stats(q_ref[0, at, col], averager)
            q = (normed * gain_ref[0:1, :]).astype(bf16).astype(f32) * 0.125
            normed, _unused = head_stats(k_ref[0, at, col], averager)
            k = normed * gain_ref[1:2, :]
            v = v_ref[0, at, col].astype(f32)
            g = g_ref[0, at, col].astype(f32)
            high, low = split(g * o_ref[0, at, col].astype(f32))
            centre = dot(high, crosser) + dot(low, crosser)
            centre_high = centre.astype(bf16).astype(f32)
            g_more = jnp.where(
                slot == 12, centre_high, jnp.where(slot == 13, centre - centre_high, 0.0)
            )
            v_more = jnp.where((slot == 12) | (slot == 13), -1.0, 0.0)
            qa[2 * p, at, :] = jnp.where(low_half, q, q_more).astype(bf16)
            qa[2 * p + 1, at, :] = jnp.where(low_half, q_more, q).astype(bf16)
            ka[2 * p, at, :] = jnp.where(low_half, k, k_more).astype(bf16)
            ka[2 * p + 1, at, :] = jnp.where(low_half, k_more, k).astype(bf16)
            va[2 * p, at, :] = jnp.where(low_half, v, v_more).astype(bf16)
            va[2 * p + 1, at, :] = jnp.where(low_half, v_more, v).astype(bf16)
            ga[2 * p, at, :] = jnp.where(low_half, g, g_more).astype(bf16)
            ga[2 * p + 1, at, :] = jnp.where(low_half, g_more, g).astype(bf16)
            kt[p, :, at] = k.astype(bf16).T
        return 0

    lax.fori_loop(0, blocks, prepare, 0)
    dqt[...] = jnp.zeros_like(dqt)
    stat_ref[...] = jnp.zeros_like(stat_ref)

    def pull_norm(raw, grad, gain):
        normed, rstd = head_stats(raw, averager)
        lifted = grad * gain
        mean_one = dot(lifted.astype(bf16), averager)
        mean_two = dot((lifted * normed).astype(bf16), averager)
        raw_grad = rstd * (lifted - mean_one - normed * mean_two)
        return raw_grad.astype(bf16), jnp.sum(grad * normed, axis=0, keepdims=True)

    def key_block(b, _):
        keys = pl.ds(pl.multiple_of(b * BLK, BLK), BLK)
        dk[...] = jnp.zeros_like(dk)
        dv[...] = jnp.zeros_like(dv)

        def query_block(qb, _):
            at = pl.ds(pl.multiple_of(qb * BLK, BLK), BLK)
            for h in range(heads):
                p, half = h // 2, slice((h % 2) * HD, (h % 2 + 1) * HD)
                scores = dot_nt(ka[h, keys, :], qa[h, at, :])
                probs = jnp.exp2(scores * LOG2E)
                pulls = dot_nt(va[h, keys, :], ga[h, at, :])
                grads = (probs * pulls).astype(bf16)
                dv[h] += dot(probs.astype(bf16), ga[h, at, :])
                dk[h] += dot(grads, qa[h, at, :])
                dqt[p, half, at] += dot(kt[p, half, keys], grads)
            return 0

        lax.fori_loop(bounds[row, 2, b], bounds[row, 3, b], query_block, 0)
        for p in range(GROUP):
            col = slice(p * PAIR, (p + 1) * PAIR)
            grad = jnp.where(low_half, dk[2 * p], dk[2 * p + 1])
            raw_grad, gain_grad = pull_norm(k_ref[0, keys, col], grad, gain_ref[1:2, :])
            out_ref[1, 0, keys, col] = raw_grad
            stat_ref[0, 1:2, col] += gain_grad
            stat_ref[0, 3:4, col] += jnp.sum(raw_grad.astype(f32), axis=0, keepdims=True)
            grad_v = jnp.where(low_half, dv[2 * p], dv[2 * p + 1]).astype(bf16)
            out_ref[2, 0, keys, col] = grad_v
            stat_ref[0, 4:5, col] += jnp.sum(grad_v.astype(f32), axis=0, keepdims=True)
        return 0

    lax.fori_loop(0, blocks, key_block, 0)

    def finish(b, _):
        at = pl.ds(pl.multiple_of(b * BLK, BLK), BLK)
        for p in range(GROUP):
            col = slice(p * PAIR, (p + 1) * PAIR)
            grad = dqt[p, :, at].T * 0.125
            raw_grad, gain_grad = pull_norm(q_ref[0, at, col], grad, gain_ref[0:1, :])
            out_ref[0, 0, at, col] = raw_grad
            stat_ref[0, 0:1, col] += gain_grad
            stat_ref[0, 2:3, col] += jnp.sum(raw_grad.astype(f32), axis=0, keepdims=True)
        return 0

    lax.fori_loop(0, blocks, finish, 0)


def attention(qkv, pic, bounds, gains):
    rows, slots, _ = qkv.shape
    width = qkv.shape[2] // 3
    wide = GROUP * PAIR
    groups = width // wide
    flops = rows * H * slots * slots * 256 * 4
    part = lambda i: pl.BlockSpec((1, slots, wide), lambda r, g, b: (r, 0, i * groups + g))
    whole = pl.BlockSpec((1, slots, wide), lambda r, g, b: (r, 0, g))
    return pl.pallas_call(
        forward_kernel,
        name="attention_forward",
        grid_spec=pltpu.PrefetchScalarGridSpec(
            num_scalar_prefetch=1,
            grid=(rows, groups),
            in_specs=[
                part(0),
                part(1),
                part(2),
                pl.BlockSpec((1, slots, 1), lambda r, g, b: (r, 0, 0)),
                pl.BlockSpec((2, PAIR), lambda r, g, b: (0, 0)),
            ],
            out_specs=[whole, whole],
            scratch_shapes=[
                pltpu.VMEM((2 * GROUP, slots, PAIR), bf16),
                pltpu.VMEM((2 * GROUP, slots, PAIR), bf16),
                pltpu.VMEM((2 * GROUP, slots, PAIR), bf16),
                pltpu.VMEM((2 * GROUP, BLK, PAIR), f32),
            ],
        ),
        out_shape=[
            jax.ShapeDtypeStruct((rows, slots, width), bf16),
            jax.ShapeDtypeStruct((rows, slots, width), f32),
        ],
        cost_estimate=pl.CostEstimate(
            flops=flops, bytes_accessed=rows * slots * width * 12, transcendentals=0
        ),
        compiler_params=pltpu.CompilerParams(vmem_limit_bytes=48 << 20),
    )(bounds, qkv, qkv, qkv, pic, gains)


def attention_back(qkv, attn, grad_attn, lse, pic, bounds, gains):
    rows, slots, _ = qkv.shape
    width = qkv.shape[2] // 3
    wide = GROUP * PAIR
    groups = width // wide
    flops = rows * H * slots * slots * 256 * 10
    part = lambda i: pl.BlockSpec((1, slots, wide), lambda r, g, b: (r, 0, i * groups + g))
    whole = pl.BlockSpec((1, slots, wide), lambda r, g, b: (r, 0, g))
    return pl.pallas_call(
        backward_kernel,
        name="attention_backward",
        grid_spec=pltpu.PrefetchScalarGridSpec(
            num_scalar_prefetch=1,
            grid=(rows, groups),
            in_specs=[
                part(0),
                part(1),
                part(2),
                whole,
                whole,
                whole,
                pl.BlockSpec((1, slots, 1), lambda r, g, b: (r, 0, 0)),
                pl.BlockSpec((2, PAIR), lambda r, g, b: (0, 0)),
            ],
            out_specs=[
                pl.BlockSpec((3, 1, slots, wide), lambda r, g, b: (0, r, 0, g)),
                pl.BlockSpec((1, 8, wide), lambda r, g, b: (r, 0, g)),
            ],
            scratch_shapes=[
                pltpu.VMEM((2 * GROUP, slots, PAIR), bf16),
                pltpu.VMEM((2 * GROUP, slots, PAIR), bf16),
                pltpu.VMEM((2 * GROUP, slots, PAIR), bf16),
                pltpu.VMEM((2 * GROUP, slots, PAIR), bf16),
                pltpu.VMEM((GROUP, PAIR, slots), bf16),
                pltpu.VMEM((GROUP, PAIR, slots), f32),
                pltpu.VMEM((2 * GROUP, BLK, PAIR), f32),
                pltpu.VMEM((2 * GROUP, BLK, PAIR), f32),
            ],
        ),
        out_shape=[
            jax.ShapeDtypeStruct((3, rows, slots, width), bf16),
            jax.ShapeDtypeStruct((rows, 8, width), f32),
        ],
        cost_estimate=pl.CostEstimate(
            flops=flops, bytes_accessed=rows * slots * width * 20, transcendentals=0
        ),
        compiler_params=pltpu.CompilerParams(vmem_limit_bytes=56 << 20),
    )(bounds, qkv, qkv, qkv, attn, grad_attn, lse, pic, gains)


def picture_tables(lengths, slots):
    ends = jnp.cumsum(lengths, axis=1)
    position = jnp.arange(slots, dtype=jnp.int32)
    pic = jnp.sum((position[None, :, None] >= ends[:, None, :]).astype(jnp.int32), axis=2)
    inside = (position[None, :] < ends[:, -1:]).astype(f32)
    first = jnp.arange(0, slots, BLK, dtype=jnp.int32)
    last = first + (BLK - 1)
    before = jnp.where(ends[:, None, :] <= first[None, :, None], ends[:, None, :], 0)
    begin = jnp.max(before, axis=2)
    after = jnp.where(ends[:, None, :] > last[None, :, None], ends[:, None, :], slots)
    end = jnp.min(after, axis=2)
    low = begin // BLK
    high = (end + BLK - 1) // BLK
    used = ((ends[:, -1:] + BLK - 1) // BLK) * jnp.ones_like(high)
    index = jnp.arange(slots // BLK, dtype=jnp.int32)[None, :]
    low_back = low
    high_back = jnp.where(index < used, jnp.minimum(high, used), low)
    bounds = jnp.stack([low, high, low_back, high_back], axis=1).astype(jnp.int32)
    return pic.astype(jnp.int32), inside, bounds


def norm_stats(values):
    mean = jnp.mean(values, axis=-1, keepdims=True)
    centered = values - mean
    variance = jnp.mean(centered * centered, axis=-1, keepdims=True)
    rstd = lax.rsqrt(variance + 1e-6)
    return centered * rstd, rstd


def norm_back(grad, normed, rstd, gain):
    lifted = grad * gain
    mean_one = jnp.mean(lifted, axis=-1, keepdims=True)
    mean_two = jnp.mean(lifted * normed, axis=-1, keepdims=True)
    return (
        rstd * (lifted - mean_one - normed * mean_two),
        jnp.sum(grad * normed, axis=0),
        jnp.sum(grad, axis=0),
    )


class Place:
    def __init__(self, fsdp, replicas):
        self.groups, self.rests = fsdp, replicas // 4
        dp = lax.axis_index("dp")
        self.f = lax.axis_index("fsdp")
        self.core = lax.rem(dp, 2)
        self.side = lax.rem(dp // 2, 2)
        self.rest = dp // 4

    def device(self, f=None, core=None, side=None, rest=None):
        f = self.f if f is None else f
        core = self.core if core is None else core
        side = self.side if side is None else side
        rest = self.rest if rest is None else rest
        return ((rest * 2 + side) * 2 + core, f)


def remote(src, dst, send, recv, device):
    return pltpu.make_async_remote_copy(
        src_ref=src,
        dst_ref=dst,
        send_sem=send,
        recv_sem=recv,
        device_id=device,
        device_id_type=pl.DeviceIdType.MESH,
    )


def greet(devices):
    barrier = pltpu.get_barrier_semaphore()
    for device in devices:
        pl.semaphore_signal(
            barrier, inc=1, device_id=device, device_id_type=pl.DeviceIdType.MESH
        )
    pl.semaphore_wait(barrier, len(devices))


def gather_kernel(fsdp, replicas, pieces, *refs):
    count = len(pieces)
    shards, fulls = refs[:count], refs[count : 2 * count]
    own_sem, out_send, out_recv, side_send, side_recv = refs[2 * count :]
    me = Place(fsdp, replicas)
    sibling = me.device(core=1 - me.core)
    peers = [lax.rem(me.f + k, fsdp) for k in range(1, fsdp)]
    sources = [lax.rem(me.f + fsdp - k, fsdp) for k in range(1, fsdp)]
    greet([sibling] + [me.device(f=peer) for peer in peers])
    own, outer, inner = [], [], []
    for i in range(count):
        for start, size in pieces[i]:
            col = pl.ds(start, size)
            for k, peer in enumerate(peers):
                at = len(outer)
                copy = remote(
                    shards[i].at[me.core, :, col],
                    fulls[i].at[me.f, me.core, :, col],
                    out_send.at[at],
                    out_recv.at[at],
                    me.device(f=peer),
                )
                copy.start()
                outer.append((copy, i, col, k))
    for i in range(count):
        copy = pltpu.make_async_copy(shards[i], fulls[i].at[me.f], own_sem.at[i])
        copy.start()
        own.append(copy)
    for at, (copy, i, col, k) in enumerate(outer):
        copy.wait_recv()
        landed = fulls[i].at[sources[k], me.core, :, col]
        forward = remote(landed, landed, side_send.at[at], side_recv.at[at], sibling)
        forward.start()
        inner.append(forward)
    for copy, *_ in outer:
        copy.wait_send()
    for copy in inner:
        copy.wait()
    for copy in own:
        copy.wait()


def gather_halves(fsdp, replicas, shards, pieces):
    copies = sum(len(item) for item in pieces) * (fsdp - 1)
    any_space = pl.BlockSpec(memory_space=pl.ANY)
    return pl.pallas_call(
        functools.partial(gather_kernel, fsdp, replicas, pieces),
        name="gather_halves",
        in_specs=[any_space] * len(shards),
        out_specs=[any_space] * len(shards),
        out_shape=[jax.ShapeDtypeStruct((fsdp,) + item.shape, item.dtype) for item in shards],
        scratch_shapes=[pltpu.SemaphoreType.DMA((len(shards),))]
        + [pltpu.SemaphoreType.DMA((copies,))] * 4,
        compiler_params=pltpu.CompilerParams(collective_id=1, has_side_effects=True),
    )(*shards)


def add_into(dst, sources):
    def step(i, _):
        total = sources[0][i].astype(f32)
        for item in sources[1:]:
            total = total + item[i].astype(f32)
        dst[i] = total.astype(bf16)
        return 0

    lax.fori_loop(0, dst.shape[0], step, 0)


def reduce_kernel(fsdp, replicas, count, *refs):
    grads, outs = refs[:count], refs[count : 2 * count]
    from_core = refs[2 * count : 3 * count]
    from_group = refs[3 * count : 4 * count]
    from_side = refs[4 * count : 5 * count]
    from_rest = refs[5 * count : 6 * count]
    send, recv = refs[6 * count :]
    me = Place(fsdp, replicas)
    rests = replicas // 4
    sibling = me.device(core=1 - me.core)
    across = me.device(side=1 - me.side)
    groups = [lax.rem(me.f + k, fsdp) for k in range(1, fsdp)]
    others = [lax.rem(me.rest + k, rests) for k in range(1, rests)]
    greet(
        [sibling, across]
        + [me.device(f=item) for item in groups]
        + [me.device(rest=item) for item in others]
    )
    used = [0]

    def start(src, dst, device):
        at = used[0]
        used[0] += 1
        copy = remote(src, dst, send.at[at], recv.at[at], device)
        copy.start()
        return copy

    sent = []
    flying = [None] * count

    def stage(i, number):
        if number > 0:
            for copy in flying[i]:
                copy.wait_recv()
                sent.append(copy)
        begun = []
        if number == 0:
            for f in range(fsdp):
                begun.append(
                    start(grads[i].at[f, :, :, 1 - me.core], from_core[i].at[f], sibling)
                )
        elif number == 1:
            for f in range(fsdp):
                for side in range(2):
                    add_into(
                        from_core[i].at[f, :, side],
                        [grads[i].at[f, :, side, me.core], from_core[i].at[f, :, side]],
                    )
            for k, f in enumerate(groups):
                begun.append(start(from_core[i].at[f], from_group[i].at[k], me.device(f=f)))
        elif number == 2:
            for side in range(2):
                add_into(
                    from_group[i].at[0, :, side],
                    [from_core[i].at[me.f, :, side]]
                    + [from_group[i].at[k, :, side] for k in range(fsdp - 1)],
                )
            begun.append(start(from_group[i].at[0, :, 1 - me.side], from_side[i], across))
        elif number == 3:
            add_into(from_side[i], [from_group[i].at[0, :, me.side], from_side[i]])
            for k, rest in enumerate(others):
                begun.append(
                    start(from_side[i].at[rest], from_rest[i].at[k], me.device(rest=rest))
                )
        elif number == 4:
            mine = outs[i].at[pl.ds(me.rest, 1), me.side, me.core]
            add_into(
                mine,
                [from_side[i].at[pl.ds(me.rest, 1)]]
                + [from_rest[i].at[pl.ds(k, 1)] for k in range(rests - 1)],
            )
            for rest in others:
                begun.append(start(mine, mine, me.device(rest=rest)))
        elif number == 5:
            mine = outs[i].at[:, me.side, me.core]
            begun.append(start(mine, mine, across))
        elif number == 6:
            mine = outs[i].at[:, :, me.core]
            begun.append(start(mine, mine, sibling))
        flying[i] = begun

    stages = 8
    for tick in range(stages + count - 1):
        for i in range(count):
            number = tick - i
            if 0 <= number < stages:
                stage(i, number)
    for copy in sent:
        copy.wait_send()


def reduce_everywhere(fsdp, replicas, grads):
    rests = replicas // 4
    count = len(grads)
    tails = [item.shape[-2:] for item in grads]
    copies = count * (fsdp + (fsdp - 1) + 1 + (rests - 1) + (rests - 1) + 2)
    vmem = pl.BlockSpec(memory_space=pltpu.VMEM)
    return pl.pallas_call(
        functools.partial(reduce_kernel, fsdp, replicas, count),
        name="reduce_everywhere",
        in_specs=[vmem] * count,
        out_specs=[vmem] * count,
        out_shape=[jax.ShapeDtypeStruct((rests, 2, 2) + tail, bf16) for tail in tails],
        scratch_shapes=[pltpu.VMEM((fsdp, rests, 2) + tail, bf16) for tail in tails]
        + [pltpu.VMEM((fsdp - 1, rests, 2) + tail, bf16) for tail in tails]
        + [pltpu.VMEM((rests,) + tail, bf16) for tail in tails]
        + [pltpu.VMEM((rests - 1,) + tail, bf16) for tail in tails]
        + [pltpu.SemaphoreType.DMA((copies,))] * 2,
        compiler_params=pltpu.CompilerParams(
            collective_id=2, has_side_effects=True, vmem_limit_bytes=60 << 20
        ),
    )(*grads)


GELU_C = math.sqrt(2.0 / math.pi)


def gelu_both(v):
    square = v * v
    t = jnp.tanh(GELU_C * v * (1.0 + 0.044715 * square))
    half = 0.5 * (1.0 + t)
    slope = half + 0.5 * v * (1.0 - t * t) * GELU_C * (1.0 + 3 * 0.044715 * square)
    return v * half, slope


def on_device(fsdp, replicas, *args):
    (
        patches,
        ln_gain,
        ln_bias,
        w_qkv,
        b_qkv,
        qk_gain,
        w_proj,
        out_bias,
        w_in,
        b_in,
        w_out,
        lengths,
        cotangent,
    ) = args
    rows, slots, width = patches.shape
    tokens = rows * slots
    small = (ln_gain, ln_bias, b_qkv, qk_gain, out_bias, b_in)
    flat = jnp.concatenate([item.reshape(-1) for item in small])
    small_cols = -(-flat.shape[0] // (32 * PAIR)) * PAIR
    flat = jnp.pad(flat, (0, 32 * small_cols - flat.shape[0])).reshape(2, 16, small_cols)
    shard_rows, columns = w_qkv.shape
    third = columns // 3
    w_qkv_full, flat_full = gather_halves(
        fsdp,
        replicas,
        [w_qkv.reshape(2, shard_rows // 2, columns), flat],
        [[(0, third), (third, third), (2 * third, third)], [(0, small_cols)]],
    )
    w_qkv_full = w_qkv_full.reshape(width, columns)
    flat_full, w_proj, w_in, w_out = lax.optimization_barrier((flat_full, w_proj, w_in, w_out))
    flat_full = flat_full.reshape(fsdp, -1).astype(f32)
    full_small = []
    at = 0
    for item in small:
        size = item.size
        piece = flat_full[:, at : at + size].reshape((fsdp,) + item.shape)
        at += size
        full_small.append(jnp.moveaxis(piece, 0, -2).reshape(item.shape[:-1] + (-1,)))
    gains, shifts, b_qkv_full, qk_gain_full, out_bias_full, b_in_full = full_small
    w_proj_full = lax.all_gather(w_proj, "fsdp", axis=0, tiled=True)
    w_in_full = lax.all_gather(w_in, "fsdp", axis=0, tiled=True)
    w_out_full = lax.all_gather(w_out, "fsdp", axis=0, tiled=True)

    pic, inside, bounds = picture_tables(lengths, slots)
    pic = pic[:, :, None]
    pair_gain = jnp.concatenate([qk_gain_full, qk_gain_full], axis=1)
    inside = inside.reshape(tokens, 1)

    source = patches.reshape(tokens, width).astype(f32)
    n1, rstd1 = norm_stats(source)
    normed1 = (n1 * gains[0] + shifts[0]).astype(bf16)
    qkv = (dot(normed1, w_qkv_full) + b_qkv_full).astype(bf16).reshape(rows, slots, columns)
    attn, lse = attention(qkv, pic, bounds, pair_gain)
    attn_flat = attn.reshape(tokens, width)
    resid = source + dot(attn_flat, w_proj_full) + out_bias_full[0]
    n2, rstd2 = norm_stats(resid)
    normed2 = (n2 * gains[1] + shifts[1]).astype(bf16)
    grad_y = cotangent.reshape(tokens, width).astype(f32) * inside
    grad_mlp = grad_y.astype(bf16)

    hidden = dot(normed2, w_in_full) + b_in_full
    activated, slope = gelu_both(hidden)
    activated = activated.astype(bf16)
    block_out = resid + dot(activated, w_out_full) + out_bias_full[1]
    block_out = block_out.astype(bf16)
    grad_hidden = (dot_nt(grad_mlp, w_out_full) * slope).astype(bf16)
    tt = (((0,), (0,)), ((), ()))
    grad_w_out = lax.dot_general(activated, grad_mlp, tt, preferred_element_type=f32).astype(bf16)
    grad_w_in = lax.dot_general(normed2, grad_hidden, tt, preferred_element_type=f32).astype(bf16)
    grad_b_in = jnp.sum(grad_hidden.astype(f32), axis=0)
    grad_bias_mlp = jnp.sum(grad_y, axis=0)
    grad_norm2 = dot_nt(grad_hidden, w_in_full)
    back2, grad_gain2, grad_shift2 = norm_back(grad_norm2, n2, rstd2, gains[1])
    grad_resid = grad_y + back2
    grad_branch = grad_resid.astype(bf16)
    grad_bias_attn = jnp.sum(grad_branch.astype(f32), axis=0)
    grad_attn = dot_nt(grad_branch, w_proj_full).astype(bf16)
    grad_w_proj = lax.dot_general(attn_flat, grad_branch, tt, preferred_element_type=f32).astype(bf16)

    grad_qkv, stats = attention_back(
        qkv, attn, grad_attn.reshape(rows, slots, width), lse, pic, bounds, pair_gain
    )
    stats = jnp.sum(stats, axis=0)
    grad_qk_gain = jnp.sum(stats[0:2].reshape(2, H, HD), axis=1)
    grad_b_qkv = stats[2:5].reshape(-1)
    grad_qkv = grad_qkv.reshape(3, tokens, width)
    grad_w_qkv = [
        lax.dot_general(normed1, grad_qkv[i], tt, preferred_element_type=f32).astype(bf16)
        for i in range(3)
    ]
    grad_norm1 = sum(
        dot_nt(grad_qkv[i], w_qkv_full[:, i * width : (i + 1) * width]) for i in range(3)
    )
    back1, grad_gain1, grad_shift1 = norm_back(grad_norm1, n1, rstd1, gains[0])
    grad_patches = (grad_resid + back1).reshape(rows, slots, width)

    small_grads = (
        jnp.stack([grad_gain1, grad_gain2]),
        jnp.stack([grad_shift1, grad_shift2]),
        grad_b_qkv,
        grad_qk_gain,
        jnp.stack([grad_bias_attn, grad_bias_mlp]),
        grad_b_in,
    )
    flat_grads = jnp.concatenate(
        [
            jnp.moveaxis(item.reshape(item.shape[:-1] + (fsdp, -1)), -2, 0).reshape(fsdp, -1)
            for item in small_grads
        ],
        axis=1,
    ).astype(bf16)
    lead = (fsdp, replicas // 4, 2, 2)
    hidden_blocks = w_in.shape[1] // width
    small_rows = 16
    flat_grads = jnp.pad(
        flat_grads, ((0, 0), (0, replicas * small_rows * width - flat_grads.shape[1]))
    )
    qkv_rows = jnp.stack(grad_w_qkv).reshape(3, fsdp, shard_rows, width)
    qkv_rows = jnp.swapaxes(qkv_rows, 0, 1).reshape(lead + (-1, width))
    proj_rows = grad_w_proj.reshape(lead + (-1, width))
    last_rows = [proj_rows, qkv_rows, flat_grads.reshape(lead + (small_rows, width))]
    last_sizes = [item.shape[-2] for item in last_rows]
    spare = -sum(last_sizes) % 16
    last_rows.append(jnp.zeros(lead + (spare, width), bf16))
    in_rows = grad_w_in.reshape(fsdp, shard_rows, hidden_blocks, width)
    in_rows = jnp.moveaxis(in_rows, 2, 1).reshape(lead + (-1, width))
    out_rows = grad_w_out.reshape(lead + (-1, width))
    r_out, r_in, r_last = reduce_everywhere(
        fsdp, replicas, [out_rows, in_rows, jnp.concatenate(last_rows, axis=-2)]
    )
    r_w_out = r_out.reshape(-1, width)
    r_w_in = jnp.moveaxis(r_in.reshape(hidden_blocks, shard_rows, width), 0, 1)
    r_w_in = r_w_in.reshape(shard_rows, -1)
    first, second = last_sizes[0], last_sizes[0] + last_sizes[1]
    r_w_proj = r_last[..., :first, :].reshape(-1, width)
    r_w_qkv = r_last[..., first:second, :].reshape(3, shard_rows, width)
    r_w_qkv = jnp.swapaxes(r_w_qkv, 0, 1).reshape(shard_rows, columns)
    r_flat = r_last[..., second : second + small_rows, :].reshape(-1).astype(f32)
    r_small = []
    at = 0
    for item in small:
        r_small.append(r_flat[at : at + item.size].reshape(item.shape))
        at += item.size
    return (
        block_out.reshape(rows, slots, width),
        grad_patches,
        r_small[0],
        r_small[1],
        r_w_qkv.astype(f32),
        r_small[2],
        r_small[3],
        r_w_proj.astype(f32),
        r_small[4],
        r_w_in.astype(f32),
        r_small[5],
        r_w_out.astype(f32),
    )


def solution(mesh):
    fsdp = mesh.shape["fsdp"]
    replicas = mesh.shape["dp"]
    every = ("dp", "fsdp")
    by_row = P(every, None, None)
    last, lead = P(None, "fsdp"), P("fsdp", None)
    placed = (
        by_row,
        last,
        last,
        lead,
        P("fsdp"),
        last,
        lead,
        last,
        lead,
        P("fsdp"),
        lead,
        P(every, None),
        by_row,
    )
    outs = (by_row, by_row, last, last, lead, P("fsdp"), last, lead, last, lead, P("fsdp"), lead)
    return jax.shard_map(
        functools.partial(on_device, fsdp, replicas),
        mesh=mesh,
        in_specs=placed,
        out_specs=outs,
        check_vma=False,
    )
```

```python
import functools
import math

import jax
import jax.numpy as jnp
from jax import lax
from jax.experimental import pallas as pl
from jax.experimental.pallas import tpu as pltpu
from jax.sharding import PartitionSpec as P

H = 12
HD = 64
PAIR = 2 * HD
GROUP = 3
BLK = 256
MASK = 256.0
LOG2E = math.log2(math.e)
f32 = jnp.float32
bf16 = jnp.bfloat16
NT = (((1,), (1,)), ((), ()))


def dot(a, b):
    return jnp.dot(a, b, preferred_element_type=f32)


def dot_nt(a, b):
    return lax.dot_general(a, b, NT, preferred_element_type=f32)


def lanes(rows):
    return lax.broadcasted_iota(jnp.int32, (rows, PAIR), 1)


def half_matrix(same, value):
    i = lax.broadcasted_iota(jnp.int32, (PAIR, PAIR), 0) // HD
    j = lax.broadcasted_iota(jnp.int32, (PAIR, PAIR), 1) // HD
    hit = (i == j) if same else (i != j)
    return jnp.where(hit, value, 0.0).astype(bf16)


def head_stats(raw, averager):
    mean = dot(raw, averager)
    centered = raw.astype(f32) - mean
    variance = dot((centered * centered).astype(bf16), averager)
    rstd = lax.rsqrt(variance + 1e-6)
    return centered * rstd, rstd


def split(v):
    high = v.astype(bf16)
    low = (v - high.astype(f32)).astype(bf16)
    return high, low


def query_extra(pic, lane):
    slot = lane % HD
    hot = jnp.where(slot == pic, MASK, 0.0)
    return jnp.where(slot == 11, -MASK, hot)


def key_extra(pic, lane):
    slot = lane % HD
    hot = jnp.where(slot == pic, 1.0, 0.0)
    return jnp.where(slot == 11, 1.0, jnp.where((slot == 12) | (slot == 13), -1.0, hot))


def forward_kernel(
    bounds, q_ref, k_ref, v_ref, pic_ref, gain_ref, out_ref, lse_ref, qa, ka, va, acc
):
    row = pl.program_id(0)
    slots = q_ref.shape[1]
    blocks = slots // BLK
    averager = half_matrix(True, 1.0 / HD)
    lane = lanes(BLK)
    low_half = lane < HD
    heads = 2 * GROUP

    def prepare(b, _):
        at = pl.ds(pl.multiple_of(b * BLK, BLK), BLK)
        pic = pic_ref[0, at, :]
        q_more = query_extra(pic, lane)
        k_more = key_extra(pic, lane)
        for p in range(GROUP):
            col = slice(p * PAIR, (p + 1) * PAIR)
            normed, _unused = head_stats(q_ref[0, at, col], averager)
            q = (normed * gain_ref[0:1, :]).astype(bf16).astype(f32) * 0.125
            normed, _unused = head_stats(k_ref[0, at, col], averager)
            k = normed * gain_ref[1:2, :]
            v = v_ref[0, at, col].astype(f32)
            qa[2 * p, at, :] = jnp.where(low_half, q, q_more).astype(bf16)
            qa[2 * p + 1, at, :] = jnp.where(low_half, q_more, q).astype(bf16)
            ka[2 * p, at, :] = jnp.where(low_half, k, k_more).astype(bf16)
            ka[2 * p + 1, at, :] = jnp.where(low_half, k_more, k).astype(bf16)
            va[2 * p, at, :] = jnp.where(low_half, v, 1.0).astype(bf16)
            va[2 * p + 1, at, :] = jnp.where(low_half, 1.0, v).astype(bf16)
        return 0

    lax.fori_loop(0, blocks, prepare, 0)

    def query_block(b, _):
        at = pl.ds(pl.multiple_of(b * BLK, BLK), BLK)
        acc[...] = jnp.zeros_like(acc)

        def key_block(kb, _):
            keys = pl.ds(pl.multiple_of(kb * BLK, BLK), BLK)
            for h in range(heads):
                scores = dot_nt(qa[h, at, :], ka[h, keys, :])
                probs = jnp.exp2(scores * LOG2E).astype(bf16)
                acc[h] += dot(probs, va[h, keys, :])
            return 0

        lax.fori_loop(bounds[row, 0, b], bounds[row, 1, b], key_block, 0)
        for p in range(GROUP):
            col = slice(p * PAIR, (p + 1) * PAIR)
            even, odd = acc[2 * p], acc[2 * p + 1]
            crossed = jnp.where(low_half, odd, even)
            total = pltpu.roll(crossed, HD, 1)
            out_ref[0, at, col] = (jnp.where(low_half, even, odd) / total).astype(bf16)
            lse_ref[0, at, col] = jnp.log(crossed)
        return 0

    lax.fori_loop(0, blocks, query_block, 0)


def backward_kernel(
    bounds,
    q_ref,
    k_ref,
    v_ref,
    o_ref,
    g_ref,
    lse_ref,
    pic_ref,
    gain_ref,
    out_ref,
    stat_ref,
    qa,
    ka,
    va,
    ga,
    kt,
    dqt,
    dk,
    dv,
):
    row = pl.program_id(0)
    slots = q_ref.shape[1]
    blocks = slots // BLK
    averager = half_matrix(True, 1.0 / HD)
    crosser = half_matrix(False, 1.0)
    lane = lanes(BLK)
    slot = lane % HD
    low_half = lane < HD
    heads = 2 * GROUP

    def prepare(b, _):
        at = pl.ds(pl.multiple_of(b * BLK, BLK), BLK)
        pic = pic_ref[0, at, :]
        q_hot = query_extra(pic, lane)
        k_more = key_extra(pic, lane)
        for p in range(GROUP):
            col = slice(p * PAIR, (p + 1) * PAIR)
            lse = lse_ref[0, at, col]
            lse_high = lse.astype(bf16).astype(f32)
            q_more = jnp.where(slot == 12, lse_high, jnp.where(slot == 13, lse - lse_high, q_hot))
            normed, _unused = head_stats(q_ref[0, at, col], averager)
            q = (normed * gain_ref[0:1, :]).astype(bf16).astype(f32) * 0.125
            normed, _unused = head_stats(k_ref[0, at, col], averager)
            k = normed * gain_ref[1:2, :]
            v = v_ref[0, at, col].astype(f32)
            g = g_ref[0, at, col].astype(f32)
            high, low = split(g * o_ref[0, at, col].astype(f32))
            centre = dot(high, crosser) + dot(low, crosser)
            centre_high = centre.astype(bf16).astype(f32)
            g_more = jnp.where(
                slot == 12, centre_high, jnp.where(slot == 13, centre - centre_high, 0.0)
            )
            v_more = jnp.where((slot == 12) | (slot == 13), -1.0, 0.0)
            qa[2 * p, at, :] = jnp.where(low_half, q, q_more).astype(bf16)
            qa[2 * p + 1, at, :] = jnp.where(low_half, q_more, q).astype(bf16)
            ka[2 * p, at, :] = jnp.where(low_half, k, k_more).astype(bf16)
            ka[2 * p + 1, at, :] = jnp.where(low_half, k_more, k).astype(bf16)
            va[2 * p, at, :] = jnp.where(low_half, v, v_more).astype(bf16)
            va[2 * p + 1, at, :] = jnp.where(low_half, v_more, v).astype(bf16)
            ga[2 * p, at, :] = jnp.where(low_half, g, g_more).astype(bf16)
            ga[2 * p + 1, at, :] = jnp.where(low_half, g_more, g).astype(bf16)
            kt[p, :, at] = k.astype(bf16).T
        return 0

    lax.fori_loop(0, blocks, prepare, 0)
    dqt[...] = jnp.zeros_like(dqt)
    stat_ref[...] = jnp.zeros_like(stat_ref)

    def pull_norm(raw, grad, gain):
        normed, rstd = head_stats(raw, averager)
        lifted = grad * gain
        mean_one = dot(lifted.astype(bf16), averager)
        mean_two = dot((lifted * normed).astype(bf16), averager)
        raw_grad = rstd * (lifted - mean_one - normed * mean_two)
        return raw_grad.astype(bf16), jnp.sum(grad * normed, axis=0, keepdims=True)

    def key_block(b, _):
        keys = pl.ds(pl.multiple_of(b * BLK, BLK), BLK)
        dk[...] = jnp.zeros_like(dk)
        dv[...] = jnp.zeros_like(dv)

        def query_block(qb, _):
            at = pl.ds(pl.multiple_of(qb * BLK, BLK), BLK)
            for h in range(heads):
                p, half = h // 2, slice((h % 2) * HD, (h % 2 + 1) * HD)
                scores = dot_nt(ka[h, keys, :], qa[h, at, :])
                probs = jnp.exp2(scores * LOG2E)
                pulls = dot_nt(va[h, keys, :], ga[h, at, :])
                grads = (probs * pulls).astype(bf16)
                dv[h] += dot(probs.astype(bf16), ga[h, at, :])
                dk[h] += dot(grads, qa[h, at, :])
                dqt[p, half, at] += dot(kt[p, half, keys], grads)
            return 0

        lax.fori_loop(bounds[row, 2, b], bounds[row, 3, b], query_block, 0)
        for p in range(GROUP):
            col = slice(p * PAIR, (p + 1) * PAIR)
            grad = jnp.where(low_half, dk[2 * p], dk[2 * p + 1])
            raw_grad, gain_grad = pull_norm(k_ref[0, keys, col], grad, gain_ref[1:2, :])
            out_ref[1, 0, keys, col] = raw_grad
            stat_ref[0, 1:2, col] += gain_grad
            stat_ref[0, 3:4, col] += jnp.sum(raw_grad.astype(f32), axis=0, keepdims=True)
            grad_v = jnp.where(low_half, dv[2 * p], dv[2 * p + 1]).astype(bf16)
            out_ref[2, 0, keys, col] = grad_v
            stat_ref[0, 4:5, col] += jnp.sum(grad_v.astype(f32), axis=0, keepdims=True)
        return 0

    lax.fori_loop(0, blocks, key_block, 0)

    def finish(b, _):
        at = pl.ds(pl.multiple_of(b * BLK, BLK), BLK)
        for p in range(GROUP):
            col = slice(p * PAIR, (p + 1) * PAIR)
            grad = dqt[p, :, at].T * 0.125
            raw_grad, gain_grad = pull_norm(q_ref[0, at, col], grad, gain_ref[0:1, :])
            out_ref[0, 0, at, col] = raw_grad
            stat_ref[0, 0:1, col] += gain_grad
            stat_ref[0, 2:3, col] += jnp.sum(raw_grad.astype(f32), axis=0, keepdims=True)
        return 0

    lax.fori_loop(0, blocks, finish, 0)


def attention(qkv, pic, bounds, gains):
    rows, slots, _ = qkv.shape
    width = qkv.shape[2] // 3
    wide = GROUP * PAIR
    groups = width // wide
    flops = rows * H * slots * slots * 256 * 4
    part = lambda i: pl.BlockSpec((1, slots, wide), lambda r, g, b: (r, 0, i * groups + g))
    whole = pl.BlockSpec((1, slots, wide), lambda r, g, b: (r, 0, g))
    return pl.pallas_call(
        forward_kernel,
        name="attention_forward",
        grid_spec=pltpu.PrefetchScalarGridSpec(
            num_scalar_prefetch=1,
            grid=(rows, groups),
            in_specs=[
                part(0),
                part(1),
                part(2),
                pl.BlockSpec((1, slots, 1), lambda r, g, b: (r, 0, 0)),
                pl.BlockSpec((2, PAIR), lambda r, g, b: (0, 0)),
            ],
            out_specs=[whole, whole],
            scratch_shapes=[
                pltpu.VMEM((2 * GROUP, slots, PAIR), bf16),
                pltpu.VMEM((2 * GROUP, slots, PAIR), bf16),
                pltpu.VMEM((2 * GROUP, slots, PAIR), bf16),
                pltpu.VMEM((2 * GROUP, BLK, PAIR), f32),
            ],
        ),
        out_shape=[
            jax.ShapeDtypeStruct((rows, slots, width), bf16),
            jax.ShapeDtypeStruct((rows, slots, width), f32),
        ],
        cost_estimate=pl.CostEstimate(
            flops=flops, bytes_accessed=rows * slots * width * 12, transcendentals=0
        ),
        compiler_params=pltpu.CompilerParams(vmem_limit_bytes=48 << 20),
    )(bounds, qkv, qkv, qkv, pic, gains)


def attention_back(qkv, attn, grad_attn, lse, pic, bounds, gains):
    rows, slots, _ = qkv.shape
    width = qkv.shape[2] // 3
    wide = GROUP * PAIR
    groups = width // wide
    flops = rows * H * slots * slots * 256 * 10
    part = lambda i: pl.BlockSpec((1, slots, wide), lambda r, g, b: (r, 0, i * groups + g))
    whole = pl.BlockSpec((1, slots, wide), lambda r, g, b: (r, 0, g))
    return pl.pallas_call(
        backward_kernel,
        name="attention_backward",
        grid_spec=pltpu.PrefetchScalarGridSpec(
            num_scalar_prefetch=1,
            grid=(rows, groups),
            in_specs=[
                part(0),
                part(1),
                part(2),
                whole,
                whole,
                whole,
                pl.BlockSpec((1, slots, 1), lambda r, g, b: (r, 0, 0)),
                pl.BlockSpec((2, PAIR), lambda r, g, b: (0, 0)),
            ],
            out_specs=[
                pl.BlockSpec((3, 1, slots, wide), lambda r, g, b: (0, r, 0, g)),
                pl.BlockSpec((1, 8, wide), lambda r, g, b: (r, 0, g)),
            ],
            scratch_shapes=[
                pltpu.VMEM((2 * GROUP, slots, PAIR), bf16),
                pltpu.VMEM((2 * GROUP, slots, PAIR), bf16),
                pltpu.VMEM((2 * GROUP, slots, PAIR), bf16),
                pltpu.VMEM((2 * GROUP, slots, PAIR), bf16),
                pltpu.VMEM((GROUP, PAIR, slots), bf16),
                pltpu.VMEM((GROUP, PAIR, slots), f32),
                pltpu.VMEM((2 * GROUP, BLK, PAIR), f32),
                pltpu.VMEM((2 * GROUP, BLK, PAIR), f32),
            ],
        ),
        out_shape=[
            jax.ShapeDtypeStruct((3, rows, slots, width), bf16),
            jax.ShapeDtypeStruct((rows, 8, width), f32),
        ],
        cost_estimate=pl.CostEstimate(
            flops=flops, bytes_accessed=rows * slots * width * 20, transcendentals=0
        ),
        compiler_params=pltpu.CompilerParams(vmem_limit_bytes=56 << 20),
    )(bounds, qkv, qkv, qkv, attn, grad_attn, lse, pic, gains)


def picture_tables(lengths, slots):
    ends = jnp.cumsum(lengths, axis=1)
    position = jnp.arange(slots, dtype=jnp.int32)
    pic = jnp.sum((position[None, :, None] >= ends[:, None, :]).astype(jnp.int32), axis=2)
    inside = (position[None, :] < ends[:, -1:]).astype(f32)
    first = jnp.arange(0, slots, BLK, dtype=jnp.int32)
    last = first + (BLK - 1)
    before = jnp.where(ends[:, None, :] <= first[None, :, None], ends[:, None, :], 0)
    begin = jnp.max(before, axis=2)
    after = jnp.where(ends[:, None, :] > last[None, :, None], ends[:, None, :], slots)
    end = jnp.min(after, axis=2)
    low = begin // BLK
    high = (end + BLK - 1) // BLK
    used = ((ends[:, -1:] + BLK - 1) // BLK) * jnp.ones_like(high)
    index = jnp.arange(slots // BLK, dtype=jnp.int32)[None, :]
    low_back = low
    high_back = jnp.where(index < used, jnp.minimum(high, used), low)
    bounds = jnp.stack([low, high, low_back, high_back], axis=1).astype(jnp.int32)
    return pic.astype(jnp.int32), inside, bounds


def norm_stats(values):
    mean = jnp.mean(values, axis=-1, keepdims=True)
    centered = values - mean
    variance = jnp.mean(centered * centered, axis=-1, keepdims=True)
    rstd = lax.rsqrt(variance + 1e-6)
    return centered * rstd, rstd


def norm_back(grad, normed, rstd, gain):
    lifted = grad * gain
    mean_one = jnp.mean(lifted, axis=-1, keepdims=True)
    mean_two = jnp.mean(lifted * normed, axis=-1, keepdims=True)
    return (
        rstd * (lifted - mean_one - normed * mean_two),
        jnp.sum(grad * normed, axis=0),
        jnp.sum(grad, axis=0),
    )


class Place:
    def __init__(self, fsdp, replicas):
        self.groups, self.rests = fsdp, replicas // 4
        dp = lax.axis_index("dp")
        self.f = lax.axis_index("fsdp")
        self.core = lax.rem(dp, 2)
        self.side = lax.rem(dp // 2, 2)
        self.rest = dp // 4

    def device(self, f=None, core=None, side=None, rest=None):
        f = self.f if f is None else f
        core = self.core if core is None else core
        side = self.side if side is None else side
        rest = self.rest if rest is None else rest
        return ((rest * 2 + side) * 2 + core, f)


def remote(src, dst, send, recv, device):
    return pltpu.make_async_remote_copy(
        src_ref=src,
        dst_ref=dst,
        send_sem=send,
        recv_sem=recv,
        device_id=device,
        device_id_type=pl.DeviceIdType.MESH,
    )


def greet(devices):
    barrier = pltpu.get_barrier_semaphore()
    for device in devices:
        pl.semaphore_signal(
            barrier, inc=1, device_id=device, device_id_type=pl.DeviceIdType.MESH
        )
    pl.semaphore_wait(barrier, len(devices))


def gather_kernel(fsdp, replicas, pieces, *refs):
    count = len(pieces)
    shards, fulls = refs[:count], refs[count : 2 * count]
    own_sem, out_send, out_recv, side_send, side_recv = refs[2 * count :]
    me = Place(fsdp, replicas)
    sibling = me.device(core=1 - me.core)
    peers = [lax.rem(me.f + k, fsdp) for k in range(1, fsdp)]
    sources = [lax.rem(me.f + fsdp - k, fsdp) for k in range(1, fsdp)]
    greet([sibling] + [me.device(f=peer) for peer in peers])
    own, outer, inner = [], [], []
    for i in range(count):
        for start, size in pieces[i]:
            col = pl.ds(start, size)
            for k, peer in enumerate(peers):
                at = len(outer)
                copy = remote(
                    shards[i].at[me.core, :, col],
                    fulls[i].at[me.f, me.core, :, col],
                    out_send.at[at],
                    out_recv.at[at],
                    me.device(f=peer),
                )
                copy.start()
                outer.append((copy, i, col, k))
    for i in range(count):
        copy = pltpu.make_async_copy(shards[i], fulls[i].at[me.f], own_sem.at[i])
        copy.start()
        own.append(copy)
    for at, (copy, i, col, k) in enumerate(outer):
        copy.wait_recv()
        landed = fulls[i].at[sources[k], me.core, :, col]
        forward = remote(landed, landed, side_send.at[at], side_recv.at[at], sibling)
        forward.start()
        inner.append(forward)
    for copy, *_ in outer:
        copy.wait_send()
    for copy in inner:
        copy.wait()
    for copy in own:
        copy.wait()


def gather_halves(fsdp, replicas, shards, pieces):
    copies = sum(len(item) for item in pieces) * (fsdp - 1)
    any_space = pl.BlockSpec(memory_space=pltpu.VMEM)
    return pl.pallas_call(
        functools.partial(gather_kernel, fsdp, replicas, pieces),
        name="gather_halves",
        in_specs=[any_space] * len(shards),
        out_specs=[any_space] * len(shards),
        out_shape=[jax.ShapeDtypeStruct((fsdp,) + item.shape, item.dtype) for item in shards],
        scratch_shapes=[pltpu.SemaphoreType.DMA((len(shards),))]
        + [pltpu.SemaphoreType.DMA((copies,))] * 4,
        compiler_params=pltpu.CompilerParams(collective_id=1, has_side_effects=True),
    )(*shards)


def add_into(dst, sources):
    def step(i, _):
        total = sources[0][i].astype(f32)
        for item in sources[1:]:
            total = total + item[i].astype(f32)
        dst[i] = total.astype(bf16)
        return 0

    lax.fori_loop(0, dst.shape[0], step, 0)


def reduce_kernel(fsdp, replicas, count, chunks, *refs):
    grads, outs = refs[:count], refs[count : 2 * count]
    parts = sum(len(chunk) for chunk in chunks)
    buffers = refs[2 * count : -2]
    send, recv = refs[-2:]
    me = Place(fsdp, replicas)
    rests = replicas // 4
    sibling = me.device(core=1 - me.core)
    across = me.device(side=1 - me.side)
    groups = [lax.rem(me.f + k, fsdp) for k in range(1, fsdp)]
    others = [lax.rem(me.rest + k, rests) for k in range(1, rests)]
    greet(
        [sibling, across]
        + [me.device(f=item) for item in groups]
        + [me.device(rest=item) for item in others]
    )
    used = [0]

    def start(src, dst, device):
        at = used[0]
        used[0] += 1
        copy = remote(src, dst, send.at[at], recv.at[at], device)
        copy.start()
        return copy

    sent = []
    flying = [None] * parts

    def stage(i, part, number):
        array, row, rows, col, cols = part
        window = (pl.ds(row, rows), pl.ds(col, cols))
        grad, out = grads[array], outs[array]
        from_core, from_group, from_side, from_rest = (
            buffers[i],
            buffers[parts + i],
            buffers[2 * parts + i],
            buffers[3 * parts + i],
        )
        if number > 0:
            for copy in flying[i]:
                copy.wait_recv()
                sent.append(copy)
        begun = []
        if number == 0:
            for f in range(fsdp):
                for side in range(2):
                    src = grad.at[(f, slice(None), side, 1 - me.core) + window]
                    begun.append(start(src, from_core.at[f, :, side], sibling))
        elif number == 1:
            for f in range(fsdp):
                for side in range(2):
                    src = grad.at[(f, slice(None), side, me.core) + window]
                    landed = from_core.at[f, :, side]
                    add_into(landed, [src, landed])
            for k, f in enumerate(groups):
                begun.append(start(from_core.at[f], from_group.at[k], me.device(f=f)))
        elif number == 2:
            for side in range(2):
                add_into(
                    from_group.at[0, :, side],
                    [from_core.at[me.f, :, side]]
                    + [from_group.at[k, :, side] for k in range(fsdp - 1)],
                )
            begun.append(start(from_group.at[0, :, 1 - me.side], from_side, across))
        elif number == 3:
            add_into(from_side, [from_group.at[0, :, me.side], from_side])
            for k, rest in enumerate(others):
                begun.append(start(from_side.at[rest], from_rest.at[k], me.device(rest=rest)))
        elif number == 4:
            mine = out.at[(pl.ds(me.rest, 1), me.side, me.core) + window]
            add_into(
                mine,
                [from_side.at[pl.ds(me.rest, 1)]]
                + [from_rest.at[pl.ds(k, 1)] for k in range(rests - 1)],
            )
            for rest in others:
                begun.append(start(mine, mine, me.device(rest=rest)))
        elif number == 5:
            mine = out.at[(slice(None), me.side, me.core) + window]
            begun.append(start(mine, mine, across))
        elif number == 6:
            for side in range(2):
                mine = out.at[(slice(None), side, me.core) + window]
                begun.append(start(mine, mine, sibling))
        flying[i] = begun

    stages = 8
    for tick in range(stages + len(chunks) - 1):
        i = 0
        for c, chunk in enumerate(chunks):
            number = tick - c
            for part in chunk:
                if 0 <= number < stages:
                    stage(i, part, number)
                i += 1
    for copy in sent:
        copy.wait_send()


def reduce_everywhere(fsdp, replicas, grads, chunks):
    rests = replicas // 4
    count = len(grads)
    tails = [(part[2], part[4]) for chunk in chunks for part in chunk]
    copies = len(tails) * (2 * fsdp + (fsdp - 1) + 1 + (rests - 1) + (rests - 1) + 3)
    vmem = pl.BlockSpec(memory_space=pltpu.VMEM)
    return pl.pallas_call(
        functools.partial(reduce_kernel, fsdp, replicas, count, chunks),
        name="reduce_everywhere",
        in_specs=[vmem] * count,
        out_specs=[vmem] * count,
        out_shape=[
            jax.ShapeDtypeStruct((rests, 2, 2) + item.shape[-2:], bf16) for item in grads
        ],
        scratch_shapes=[pltpu.VMEM((fsdp, rests, 2) + tail, bf16) for tail in tails]
        + [pltpu.VMEM((fsdp - 1, rests, 2) + tail, bf16) for tail in tails]
        + [pltpu.VMEM((rests,) + tail, bf16) for tail in tails]
        + [pltpu.VMEM((rests - 1,) + tail, bf16) for tail in tails]
        + [pltpu.SemaphoreType.DMA((copies,))] * 2,
        compiler_params=pltpu.CompilerParams(
            collective_id=2, has_side_effects=True, vmem_limit_bytes=60 << 20
        ),
    )(*grads)


GELU_C = math.sqrt(2.0 / math.pi)


def gelu_both(v):
    square = v * v
    t = jnp.tanh(GELU_C * v * (1.0 + 0.044715 * square))
    half = 0.5 * (1.0 + t)
    slope = half + 0.5 * v * (1.0 - t * t) * GELU_C * (1.0 + 3 * 0.044715 * square)
    return v * half, slope


def on_device(fsdp, replicas, *args):
    (
        patches,
        ln_gain,
        ln_bias,
        w_qkv,
        b_qkv,
        qk_gain,
        w_proj,
        out_bias,
        w_in,
        b_in,
        w_out,
        lengths,
        cotangent,
    ) = args
    rows, slots, width = patches.shape
    tokens = rows * slots
    small = (ln_gain, ln_bias, b_qkv, qk_gain, out_bias, b_in)
    flat = jnp.concatenate([item.reshape(-1) for item in small])
    small_cols = -(-flat.shape[0] // (32 * PAIR)) * PAIR
    flat = jnp.pad(flat, (0, 32 * small_cols - flat.shape[0])).reshape(2, 16, small_cols)
    shard_rows, columns = w_qkv.shape
    third = columns // 3
    w_qkv_full, flat_full = gather_halves(
        fsdp,
        replicas,
        [w_qkv.reshape(2, shard_rows // 2, columns), flat],
        [[(0, third), (third, third), (2 * third, third)], [(0, small_cols)]],
    )
    w_qkv_full = w_qkv_full.reshape(width, columns)
    flat_full, w_proj, w_in, w_out = lax.optimization_barrier((flat_full, w_proj, w_in, w_out))
    flat_full = flat_full.reshape(fsdp, -1).astype(f32)
    full_small = []
    at = 0
    for item in small:
        size = item.size
        piece = flat_full[:, at : at + size].reshape((fsdp,) + item.shape)
        at += size
        full_small.append(jnp.moveaxis(piece, 0, -2).reshape(item.shape[:-1] + (-1,)))
    gains, shifts, b_qkv_full, qk_gain_full, out_bias_full, b_in_full = full_small
    w_proj_full = lax.all_gather(w_proj, "fsdp", axis=0, tiled=True)
    w_in_full = lax.all_gather(w_in, "fsdp", axis=0, tiled=True)
    w_out_full = lax.all_gather(w_out, "fsdp", axis=0, tiled=True)

    pic, inside, bounds = picture_tables(lengths, slots)
    pic = pic[:, :, None]
    pair_gain = jnp.concatenate([qk_gain_full, qk_gain_full], axis=1)
    inside = inside.reshape(tokens, 1)

    source = patches.reshape(tokens, width).astype(f32)
    n1, rstd1 = norm_stats(source)
    normed1 = (n1 * gains[0] + shifts[0]).astype(bf16)
    qkv = (dot(normed1, w_qkv_full) + b_qkv_full).astype(bf16).reshape(rows, slots, columns)
    attn, lse = attention(qkv, pic, bounds, pair_gain)
    attn_flat = attn.reshape(tokens, width)
    resid = source + dot(attn_flat, w_proj_full) + out_bias_full[0]
    n2, rstd2 = norm_stats(resid)
    normed2 = (n2 * gains[1] + shifts[1]).astype(bf16)
    grad_y = cotangent.reshape(tokens, width).astype(f32) * inside
    grad_mlp = grad_y.astype(bf16)

    hidden = dot(normed2, w_in_full) + b_in_full
    activated, slope = gelu_both(hidden)
    activated = activated.astype(bf16)
    block_out = resid + dot(activated, w_out_full) + out_bias_full[1]
    block_out = block_out.astype(bf16)
    grad_hidden = (dot_nt(grad_mlp, w_out_full) * slope).astype(bf16)
    tt = (((0,), (0,)), ((), ()))
    grad_w_out = lax.dot_general(activated, grad_mlp, tt, preferred_element_type=f32).astype(bf16)
    grad_w_in = lax.dot_general(normed2, grad_hidden, tt, preferred_element_type=f32).astype(bf16)
    grad_b_in = jnp.sum(grad_hidden.astype(f32), axis=0)
    grad_bias_mlp = jnp.sum(grad_y, axis=0)
    grad_norm2 = dot_nt(grad_hidden, w_in_full)
    back2, grad_gain2, grad_shift2 = norm_back(grad_norm2, n2, rstd2, gains[1])
    grad_resid = grad_y + back2
    grad_branch = grad_resid.astype(bf16)
    grad_bias_attn = jnp.sum(grad_branch.astype(f32), axis=0)
    grad_attn = dot_nt(grad_branch, w_proj_full).astype(bf16)
    grad_w_proj = lax.dot_general(attn_flat, grad_branch, tt, preferred_element_type=f32).astype(bf16)

    grad_qkv, stats = attention_back(
        qkv, attn, grad_attn.reshape(rows, slots, width), lse, pic, bounds, pair_gain
    )
    stats = jnp.sum(stats, axis=0)
    grad_qk_gain = jnp.sum(stats[0:2].reshape(2, H, HD), axis=1)
    grad_b_qkv = stats[2:5].reshape(-1)
    grad_qkv = grad_qkv.reshape(3, tokens, width)
    grad_w_qkv = [
        lax.dot_general(normed1, grad_qkv[i], tt, preferred_element_type=f32).astype(bf16)
        for i in range(3)
    ]
    grad_norm1 = sum(
        dot_nt(grad_qkv[i], w_qkv_full[:, i * width : (i + 1) * width]) for i in range(3)
    )
    back1, grad_gain1, grad_shift1 = norm_back(grad_norm1, n1, rstd1, gains[0])
    grad_patches = (grad_resid + back1).reshape(rows, slots, width)

    small_grads = (
        jnp.stack([grad_gain1, grad_gain2]),
        jnp.stack([grad_shift1, grad_shift2]),
        grad_b_qkv,
        grad_qk_gain,
        jnp.stack([grad_bias_attn, grad_bias_mlp]),
        grad_b_in,
    )
    flat_grads = jnp.concatenate(
        [
            jnp.moveaxis(item.reshape(item.shape[:-1] + (fsdp, -1)), -2, 0).reshape(fsdp, -1)
            for item in small_grads
        ],
        axis=1,
    ).astype(bf16)
    lead = (fsdp, replicas // 4, 2, 2)
    small_rows = 16
    flat_grads = jnp.pad(
        flat_grads, ((0, 0), (0, replicas * small_rows * PAIR - flat_grads.shape[1]))
    )
    payload = [grad_w_out, grad_w_in, *grad_w_qkv, grad_w_proj]
    payload = [item.reshape(lead + (-1, item.shape[-1])) for item in payload]
    payload.append(flat_grads.reshape(lead + (small_rows, PAIR)))
    whole = [(i, 0, item.shape[-2], 0, item.shape[-1]) for i, item in enumerate(payload)]
    out_half, in_half = whole[0][2] // 2, whole[1][4] // 2
    out_chunks = [[whole[0]]]
    if out_half % 16 == 0:
        out_chunks = [[(0, at, out_half, 0, width)] for at in (0, out_half)]
    in_chunks = [[(1, 0, whole[1][2], at, in_half)] for at in (0, in_half)]
    chunks = out_chunks + in_chunks + [[whole[2], whole[3]], [whole[4], whole[5], whole[6]]]
    reduced = reduce_everywhere(fsdp, replicas, payload, chunks)
    r_w_out, r_w_in, r_q, r_k, r_v, r_w_proj = (
        item.reshape(-1, item.shape[-1]) for item in reduced[:6]
    )
    r_w_qkv = jnp.concatenate([r_q, r_k, r_v], axis=1)
    r_flat = reduced[6].reshape(-1).astype(f32)
    r_small = []
    at = 0
    for item in small:
        r_small.append(r_flat[at : at + item.size].reshape(item.shape))
        at += item.size
    return (
        block_out.reshape(rows, slots, width),
        grad_patches,
        r_small[0],
        r_small[1],
        r_w_qkv.astype(f32),
        r_small[2],
        r_small[3],
        r_w_proj.astype(f32),
        r_small[4],
        r_w_in.astype(f32),
        r_small[5],
        r_w_out.astype(f32),
    )


def solution(mesh):
    fsdp = mesh.shape["fsdp"]
    replicas = mesh.shape["dp"]
    every = ("dp", "fsdp")
    by_row = P(every, None, None)
    last, lead = P(None, "fsdp"), P("fsdp", None)
    placed = (
        by_row,
        last,
        last,
        lead,
        P("fsdp"),
        last,
        lead,
        last,
        lead,
        P("fsdp"),
        lead,
        P(every, None),
        by_row,
    )
    outs = (by_row, by_row, last, last, lead, P("fsdp"), last, lead, last, lead, P("fsdp"), lead)
    return jax.shard_map(
        functools.partial(on_device, fsdp, replicas),
        mesh=mesh,
        in_specs=placed,
        out_specs=outs,
        check_vma=False,
    )
```

```python
import functools
import math

import jax
import jax.numpy as jnp
from jax import lax
from jax.experimental import pallas as pl
from jax.experimental.pallas import tpu as pltpu
from jax.sharding import PartitionSpec as P

H = 12
HD = 64
PAIR = 2 * HD
GROUP = 6
BLK = 256
MASK = 256.0
LOG2E = math.log2(math.e)
f32 = jnp.float32
bf16 = jnp.bfloat16
NT = (((1,), (1,)), ((), ()))


def dot(a, b):
    return jnp.dot(a, b, preferred_element_type=f32)


def dot_nt(a, b):
    return lax.dot_general(a, b, NT, preferred_element_type=f32)


def lanes(rows):
    return lax.broadcasted_iota(jnp.int32, (rows, PAIR), 1)


def half_matrix(same, value):
    i = lax.broadcasted_iota(jnp.int32, (PAIR, PAIR), 0) // HD
    j = lax.broadcasted_iota(jnp.int32, (PAIR, PAIR), 1) // HD
    hit = (i == j) if same else (i != j)
    return jnp.where(hit, value, 0.0).astype(bf16)


def head_stats(raws, averager):
    means = [dot(raw, averager) for raw in raws]
    centered = [raw.astype(f32) - mean for raw, mean in zip(raws, means)]
    variances = [dot((item * item).astype(bf16), averager) for item in centered]
    rstds = [lax.rsqrt(item + 1e-6) for item in variances]
    return [item * rstd for item, rstd in zip(centered, rstds)], rstds


def split(v):
    high = v.astype(bf16)
    low = (v - high.astype(f32)).astype(bf16)
    return high, low


def query_extra(pic, lane):
    slot = lane % HD
    hot = jnp.where(slot == pic, MASK, 0.0)
    return jnp.where(slot == 11, -MASK, hot)


def key_extra(pic, lane):
    slot = lane % HD
    hot = jnp.where(slot == pic, 1.0, 0.0)
    return jnp.where(slot == 11, 1.0, jnp.where((slot == 12) | (slot == 13), -1.0, hot))


def forward_kernel(
    bounds, q_ref, k_ref, v_ref, pic_ref, gain_ref, out_ref, lse_ref, qa, ka, va, acc
):
    row = pl.program_id(0)
    slots = q_ref.shape[1]
    blocks = slots // BLK
    averager = half_matrix(True, 1.0 / HD)
    lane = lanes(BLK)
    low_half = lane < HD
    heads = 2 * GROUP

    def prepare(b, _):
        at = pl.ds(pl.multiple_of(b * BLK, BLK), BLK)
        pic = pic_ref[0, at, :]
        q_more = query_extra(pic, lane)
        k_more = key_extra(pic, lane)
        cols = [slice(p * PAIR, (p + 1) * PAIR) for p in range(GROUP)]
        raws = [q_ref[0, at, col] for col in cols] + [k_ref[0, at, col] for col in cols]
        normed, _unused = head_stats(raws, averager)
        for p, col in enumerate(cols):
            q = (normed[p] * gain_ref[0:1, :]).astype(bf16).astype(f32) * 0.125
            k = normed[GROUP + p] * gain_ref[1:2, :]
            v = v_ref[0, at, col].astype(f32)
            qa[2 * p, at, :] = jnp.where(low_half, q, q_more).astype(bf16)
            qa[2 * p + 1, at, :] = jnp.where(low_half, q_more, q).astype(bf16)
            ka[2 * p, at, :] = jnp.where(low_half, k, k_more).astype(bf16)
            ka[2 * p + 1, at, :] = jnp.where(low_half, k_more, k).astype(bf16)
            va[2 * p, at, :] = jnp.where(low_half, v, 1.0).astype(bf16)
            va[2 * p + 1, at, :] = jnp.where(low_half, 1.0, v).astype(bf16)
        return 0

    lax.fori_loop(0, blocks, prepare, 0)

    def query_block(b, _):
        at = pl.ds(pl.multiple_of(b * BLK, BLK), BLK)
        acc[...] = jnp.zeros_like(acc)

        def key_block(kb, _):
            keys = pl.ds(pl.multiple_of(kb * BLK, BLK), BLK)
            ahead = [dot_nt(qa[0, at, :], ka[0, keys, :])]
            for h in range(heads):
                if h + 1 < heads:
                    ahead.append(dot_nt(qa[h + 1, at, :], ka[h + 1, keys, :]))
                probs = jnp.exp2(ahead[h] * LOG2E).astype(bf16)
                acc[h] += dot(probs, va[h, keys, :])
            return 0

        lax.fori_loop(bounds[row, 0, b], bounds[row, 1, b], key_block, 0)
        for p in range(GROUP):
            col = slice(p * PAIR, (p + 1) * PAIR)
            even, odd = acc[2 * p], acc[2 * p + 1]
            crossed = jnp.where(low_half, odd, even)
            total = pltpu.roll(crossed, HD, 1)
            out_ref[0, at, col] = (jnp.where(low_half, even, odd) / total).astype(bf16)
            lse_ref[0, at, col] = jnp.log(crossed)
        return 0

    lax.fori_loop(0, blocks, query_block, 0)


def backward_kernel(
    bounds,
    q_ref,
    k_ref,
    v_ref,
    o_ref,
    g_ref,
    lse_ref,
    pic_ref,
    gain_ref,
    out_ref,
    stat_ref,
    qa,
    ka,
    va,
    ga,
    kt,
    dqt,
    dk,
    dv,
):
    row = pl.program_id(0)
    slots = q_ref.shape[1]
    blocks = slots // BLK
    averager = half_matrix(True, 1.0 / HD)
    crosser = half_matrix(False, 1.0)
    lane = lanes(BLK)
    slot = lane % HD
    low_half = lane < HD
    heads = 2 * GROUP

    def prepare(b, _):
        at = pl.ds(pl.multiple_of(b * BLK, BLK), BLK)
        pic = pic_ref[0, at, :]
        q_hot = query_extra(pic, lane)
        k_more = key_extra(pic, lane)
        cols = [slice(p * PAIR, (p + 1) * PAIR) for p in range(GROUP)]
        raws = [q_ref[0, at, col] for col in cols] + [k_ref[0, at, col] for col in cols]
        normed, _unused = head_stats(raws, averager)
        grads = [g_ref[0, at, col].astype(f32) for col in cols]
        parts = [split(g * o_ref[0, at, col].astype(f32)) for g, col in zip(grads, cols)]
        centres = [dot(high, crosser) + dot(low, crosser) for high, low in parts]
        for p, col in enumerate(cols):
            lse = lse_ref[0, at, col]
            lse_high = lse.astype(bf16).astype(f32)
            q_more = jnp.where(slot == 12, lse_high, jnp.where(slot == 13, lse - lse_high, q_hot))
            q = (normed[p] * gain_ref[0:1, :]).astype(bf16).astype(f32) * 0.125
            k = normed[GROUP + p] * gain_ref[1:2, :]
            v = v_ref[0, at, col].astype(f32)
            g, centre = grads[p], centres[p]
            centre_high = centre.astype(bf16).astype(f32)
            g_more = jnp.where(
                slot == 12, centre_high, jnp.where(slot == 13, centre - centre_high, 0.0)
            )
            v_more = jnp.where((slot == 12) | (slot == 13), -1.0, 0.0)
            qa[2 * p, at, :] = jnp.where(low_half, q, q_more).astype(bf16)
            qa[2 * p + 1, at, :] = jnp.where(low_half, q_more, q).astype(bf16)
            ka[2 * p, at, :] = jnp.where(low_half, k, k_more).astype(bf16)
            ka[2 * p + 1, at, :] = jnp.where(low_half, k_more, k).astype(bf16)
            va[2 * p, at, :] = jnp.where(low_half, v, v_more).astype(bf16)
            va[2 * p + 1, at, :] = jnp.where(low_half, v_more, v).astype(bf16)
            ga[2 * p, at, :] = jnp.where(low_half, g, g_more).astype(bf16)
            ga[2 * p + 1, at, :] = jnp.where(low_half, g_more, g).astype(bf16)
            kt[p, :, at] = k.astype(bf16).T
        return 0

    lax.fori_loop(0, blocks, prepare, 0)
    dqt[...] = jnp.zeros_like(dqt)
    stat_ref[...] = jnp.zeros_like(stat_ref)

    cols = [slice(p * PAIR, (p + 1) * PAIR) for p in range(GROUP)]

    def pull_norm(raws, grads, gain):
        normed, rstds = head_stats(raws, averager)
        lifted = [grad * gain for grad in grads]
        ones = [dot(item.astype(bf16), averager) for item in lifted]
        twos = [dot((a * n).astype(bf16), averager) for a, n in zip(lifted, normed)]
        raw_grads = [
            (rstd * (a - one - n * two)).astype(bf16)
            for rstd, a, one, n, two in zip(rstds, lifted, ones, normed, twos)
        ]
        return raw_grads, [
            jnp.sum(grad * n, axis=0, keepdims=True) for grad, n in zip(grads, normed)
        ]

    def key_block(b, _):
        keys = pl.ds(pl.multiple_of(b * BLK, BLK), BLK)
        dk[...] = jnp.zeros_like(dk)
        dv[...] = jnp.zeros_like(dv)

        def query_block(qb, _):
            at = pl.ds(pl.multiple_of(qb * BLK, BLK), BLK)
            def first(h):
                return (
                    dot_nt(ka[h, keys, :], qa[h, at, :]),
                    dot_nt(va[h, keys, :], ga[h, at, :]),
                )

            ahead = [first(0)]
            for h in range(heads):
                p, half = h // 2, slice((h % 2) * HD, (h % 2 + 1) * HD)
                if h + 1 < heads:
                    ahead.append(first(h + 1))
                scores, pulls = ahead[h]
                probs = jnp.exp2(scores * LOG2E)
                grads = (probs * pulls).astype(bf16)
                dv[h] += dot(probs.astype(bf16), ga[h, at, :])
                dk[h] += dot(grads, qa[h, at, :])
                dqt[p, half, at] += dot(kt[p, half, keys], grads)
            return 0

        lax.fori_loop(bounds[row, 2, b], bounds[row, 3, b], query_block, 0)
        grads = [jnp.where(low_half, dk[2 * p], dk[2 * p + 1]) for p in range(GROUP)]
        raw_grads, gain_grads = pull_norm(
            [k_ref[0, keys, col] for col in cols], grads, gain_ref[1:2, :]
        )
        for p, col in enumerate(cols):
            raw_grad = raw_grads[p]
            out_ref[1, 0, keys, col] = raw_grad
            stat_ref[0, 1:2, col] += gain_grads[p]
            stat_ref[0, 3:4, col] += jnp.sum(raw_grad.astype(f32), axis=0, keepdims=True)
            grad_v = jnp.where(low_half, dv[2 * p], dv[2 * p + 1]).astype(bf16)
            out_ref[2, 0, keys, col] = grad_v
            stat_ref[0, 4:5, col] += jnp.sum(grad_v.astype(f32), axis=0, keepdims=True)
        return 0

    lax.fori_loop(0, blocks, key_block, 0)

    def finish(b, _):
        at = pl.ds(pl.multiple_of(b * BLK, BLK), BLK)
        grads = [dqt[p, :, at].T * 0.125 for p in range(GROUP)]
        raw_grads, gain_grads = pull_norm(
            [q_ref[0, at, col] for col in cols], grads, gain_ref[0:1, :]
        )
        for p, col in enumerate(cols):
            raw_grad = raw_grads[p]
            out_ref[0, 0, at, col] = raw_grad
            stat_ref[0, 0:1, col] += gain_grads[p]
            stat_ref[0, 2:3, col] += jnp.sum(raw_grad.astype(f32), axis=0, keepdims=True)
        return 0

    lax.fori_loop(0, blocks, finish, 0)


def attention(qkv, pic, bounds, gains):
    rows, slots, _ = qkv.shape
    width = qkv.shape[2] // 3
    wide = GROUP * PAIR
    groups = width // wide
    flops = rows * H * slots * slots * 256 * 4
    part = lambda i: pl.BlockSpec((1, slots, wide), lambda r, g, b: (r, 0, i * groups + g))
    whole = pl.BlockSpec((1, slots, wide), lambda r, g, b: (r, 0, g))
    return pl.pallas_call(
        forward_kernel,
        name="attention_forward",
        grid_spec=pltpu.PrefetchScalarGridSpec(
            num_scalar_prefetch=1,
            grid=(rows, groups),
            in_specs=[
                part(0),
                part(1),
                part(2),
                pl.BlockSpec((1, slots, 1), lambda r, g, b: (r, 0, 0)),
                pl.BlockSpec((2, PAIR), lambda r, g, b: (0, 0)),
            ],
            out_specs=[whole, whole],
            scratch_shapes=[
                pltpu.VMEM((2 * GROUP, slots, PAIR), bf16),
                pltpu.VMEM((2 * GROUP, slots, PAIR), bf16),
                pltpu.VMEM((2 * GROUP, slots, PAIR), bf16),
                pltpu.VMEM((2 * GROUP, BLK, PAIR), f32),
            ],
        ),
        out_shape=[
            jax.ShapeDtypeStruct((rows, slots, width), bf16),
            jax.ShapeDtypeStruct((rows, slots, width), f32),
        ],
        cost_estimate=pl.CostEstimate(
            flops=flops, bytes_accessed=rows * slots * width * 12, transcendentals=0
        ),
        compiler_params=pltpu.CompilerParams(vmem_limit_bytes=48 << 20),
    )(bounds, qkv, qkv, qkv, pic, gains)


def attention_back(qkv, attn, grad_attn, lse, pic, bounds, gains):
    rows, slots, _ = qkv.shape
    width = qkv.shape[2] // 3
    wide = GROUP * PAIR
    groups = width // wide
    flops = rows * H * slots * slots * 256 * 10
    part = lambda i: pl.BlockSpec((1, slots, wide), lambda r, g, b: (r, 0, i * groups + g))
    whole = pl.BlockSpec((1, slots, wide), lambda r, g, b: (r, 0, g))
    return pl.pallas_call(
        backward_kernel,
        name="attention_backward",
        grid_spec=pltpu.PrefetchScalarGridSpec(
            num_scalar_prefetch=1,
            grid=(rows, groups),
            in_specs=[
                part(0),
                part(1),
                part(2),
                whole,
                whole,
                whole,
                pl.BlockSpec((1, slots, 1), lambda r, g, b: (r, 0, 0)),
                pl.BlockSpec((2, PAIR), lambda r, g, b: (0, 0)),
            ],
            out_specs=[
                pl.BlockSpec((3, 1, slots, wide), lambda r, g, b: (0, r, 0, g)),
                pl.BlockSpec((1, 8, wide), lambda r, g, b: (r, 0, g)),
            ],
            scratch_shapes=[
                pltpu.VMEM((2 * GROUP, slots, PAIR), bf16),
                pltpu.VMEM((2 * GROUP, slots, PAIR), bf16),
                pltpu.VMEM((2 * GROUP, slots, PAIR), bf16),
                pltpu.VMEM((2 * GROUP, slots, PAIR), bf16),
                pltpu.VMEM((GROUP, PAIR, slots), bf16),
                pltpu.VMEM((GROUP, PAIR, slots), f32),
                pltpu.VMEM((2 * GROUP, BLK, PAIR), f32),
                pltpu.VMEM((2 * GROUP, BLK, PAIR), f32),
            ],
        ),
        out_shape=[
            jax.ShapeDtypeStruct((3, rows, slots, width), bf16),
            jax.ShapeDtypeStruct((rows, 8, width), f32),
        ],
        cost_estimate=pl.CostEstimate(
            flops=flops, bytes_accessed=rows * slots * width * 20, transcendentals=0
        ),
        compiler_params=pltpu.CompilerParams(vmem_limit_bytes=56 << 20),
    )(bounds, qkv, qkv, qkv, attn, grad_attn, lse, pic, gains)


def picture_tables(lengths, slots):
    ends = jnp.cumsum(lengths, axis=1)
    position = jnp.arange(slots, dtype=jnp.int32)
    pic = jnp.sum((position[None, :, None] >= ends[:, None, :]).astype(jnp.int32), axis=2)
    inside = (position[None, :] < ends[:, -1:]).astype(f32)
    first = jnp.arange(0, slots, BLK, dtype=jnp.int32)
    last = first + (BLK - 1)
    before = jnp.where(ends[:, None, :] <= first[None, :, None], ends[:, None, :], 0)
    begin = jnp.max(before, axis=2)
    after = jnp.where(ends[:, None, :] > last[None, :, None], ends[:, None, :], slots)
    end = jnp.min(after, axis=2)
    low = begin // BLK
    high = (end + BLK - 1) // BLK
    used = ((ends[:, -1:] + BLK - 1) // BLK) * jnp.ones_like(high)
    index = jnp.arange(slots // BLK, dtype=jnp.int32)[None, :]
    low_back = low
    high_back = jnp.where(index < used, jnp.minimum(high, used), low)
    bounds = jnp.stack([low, high, low_back, high_back], axis=1).astype(jnp.int32)
    return pic.astype(jnp.int32), inside, bounds


def norm_stats(values):
    mean = jnp.mean(values, axis=-1, keepdims=True)
    centered = values - mean
    variance = jnp.mean(centered * centered, axis=-1, keepdims=True)
    rstd = lax.rsqrt(variance + 1e-6)
    return centered * rstd, rstd


def norm_back(grad, normed, rstd, gain):
    lifted = grad * gain
    mean_one = jnp.mean(lifted, axis=-1, keepdims=True)
    mean_two = jnp.mean(lifted * normed, axis=-1, keepdims=True)
    return (
        rstd * (lifted - mean_one - normed * mean_two),
        jnp.sum(grad * normed, axis=0),
        jnp.sum(grad, axis=0),
    )


class Place:
    def __init__(self, fsdp, replicas):
        self.groups, self.rests = fsdp, replicas // 4
        dp = lax.axis_index("dp")
        self.f = lax.axis_index("fsdp")
        self.core = lax.rem(dp, 2)
        self.side = lax.rem(dp // 2, 2)
        self.rest = dp // 4

    def device(self, f=None, core=None, side=None, rest=None):
        f = self.f if f is None else f
        core = self.core if core is None else core
        side = self.side if side is None else side
        rest = self.rest if rest is None else rest
        return ((rest * 2 + side) * 2 + core, f)


def remote(src, dst, send, recv, device):
    return pltpu.make_async_remote_copy(
        src_ref=src,
        dst_ref=dst,
        send_sem=send,
        recv_sem=recv,
        device_id=device,
        device_id_type=pl.DeviceIdType.MESH,
    )


def greet(devices):
    barrier = pltpu.get_barrier_semaphore()
    for device in devices:
        pl.semaphore_signal(
            barrier, inc=1, device_id=device, device_id_type=pl.DeviceIdType.MESH
        )
    pl.semaphore_wait(barrier, len(devices))


def gather_kernel(fsdp, replicas, pieces, *refs):
    count = len(pieces)
    shards, fulls = refs[:count], refs[count : 2 * count]
    own_sem, sends, recvs = refs[2 * count :]
    me = Place(fsdp, replicas)
    sibling = me.device(core=1 - me.core)
    across = me.device(side=1 - me.side)
    peers = [lax.rem(me.f + k, fsdp) for k in range(1, fsdp)]
    sources = [lax.rem(me.f + fsdp - k, fsdp) for k in range(1, fsdp)]
    greet([sibling, across] + [me.device(f=peer) for peer in peers])
    outer, crossing, inner = [], [], []
    for i in range(count):
        for start, size in pieces[i]:
            col = pl.ds(start, size)
            for k, peer in enumerate(peers):
                at = len(outer)
                copy = remote(
                    shards[i].at[me.side, me.core, :, col],
                    fulls[i].at[me.f, me.side, me.core, :, col],
                    sends.at[0, at],
                    recvs.at[0, at],
                    me.device(f=peer),
                )
                copy.start()
                outer.append((copy, i, col, k))
    own = []
    for i in range(count):
        copy = pltpu.make_async_copy(shards[i], fulls[i].at[me.f], own_sem.at[i])
        copy.start()
        own.append(copy)

    def forward(landed, kind, at, device):
        copy = remote(landed, landed, sends.at[kind, at], recvs.at[kind, at], device)
        copy.start()
        return copy

    for at in range(len(outer) + 1):
        if at < len(outer):
            copy, i, col, k = outer[at]
            copy.wait_recv()
            landed = fulls[i].at[sources[k], me.side, me.core, :, col]
            crossing.append(forward(landed, 1, at, across))
            inner.append(forward(landed, 2, at, sibling))
        if at > 0:
            _unused, i, col, k = outer[at - 1]
            crossing[at - 1].wait_recv()
            landed = fulls[i].at[sources[k], 1 - me.side, me.core, :, col]
            inner.append(forward(landed, 3, at - 1, sibling))
    for copy, *_unused in outer:
        copy.wait_send()
    for copy in crossing:
        copy.wait_send()
    for copy in inner:
        copy.wait()
    for copy in own:
        copy.wait()


def gather_quarters(fsdp, replicas, shards, pieces):
    copies = sum(len(item) for item in pieces) * (fsdp - 1)
    vmem = pl.BlockSpec(memory_space=pltpu.VMEM)
    return pl.pallas_call(
        functools.partial(gather_kernel, fsdp, replicas, pieces),
        name="gather_quarters",
        in_specs=[vmem] * len(shards),
        out_specs=[vmem] * len(shards),
        out_shape=[jax.ShapeDtypeStruct((fsdp,) + item.shape, item.dtype) for item in shards],
        scratch_shapes=[pltpu.SemaphoreType.DMA((len(shards),))]
        + [pltpu.SemaphoreType.DMA((4, copies))] * 2,
        compiler_params=pltpu.CompilerParams(
            collective_id=1, has_side_effects=True, vmem_limit_bytes=32 << 20
        ),
    )(*shards)


def add_into(dst, sources):
    def step(i, _):
        total = sources[0][i].astype(f32)
        for item in sources[1:]:
            total = total + item[i].astype(f32)
        dst[i] = total.astype(bf16)
        return 0

    lax.fori_loop(0, dst.shape[0], step, 0)


def reduce_kernel(fsdp, replicas, count, chunks, *refs):
    grads, outs = refs[:count], refs[count : 2 * count]
    parts = sum(len(chunk) for chunk in chunks)
    buffers = refs[2 * count : -2]
    send, recv = refs[-2:]
    me = Place(fsdp, replicas)
    rests = replicas // 4
    sibling = me.device(core=1 - me.core)
    across = me.device(side=1 - me.side)
    groups = [lax.rem(me.f + k, fsdp) for k in range(1, fsdp)]
    others = [lax.rem(me.rest + k, rests) for k in range(1, rests)]
    greet(
        [sibling, across]
        + [me.device(f=item) for item in groups]
        + [me.device(rest=item) for item in others]
    )
    used = [0]

    def start(src, dst, device):
        at = used[0]
        used[0] += 1
        copy = remote(src, dst, send.at[at], recv.at[at], device)
        copy.start()
        return copy

    sent = []
    flying = [None] * parts

    def stage(i, part, number):
        array, row, rows, col, cols = part
        window = (pl.ds(row, rows), pl.ds(col, cols))
        grad, out = grads[array], outs[array]
        from_core, from_group, from_side, from_rest = (
            buffers[i],
            buffers[parts + i],
            buffers[2 * parts + i],
            buffers[3 * parts + i],
        )
        if number > 0:
            for copy in flying[i]:
                copy.wait_recv()
                sent.append(copy)
        begun = []
        if number == 0:
            for f in range(fsdp):
                for side in range(2):
                    src = grad.at[(f, slice(None), side, 1 - me.core) + window]
                    begun.append(start(src, from_core.at[f, :, side], sibling))
        elif number == 1:
            for f in range(fsdp):
                for side in range(2):
                    src = grad.at[(f, slice(None), side, me.core) + window]
                    landed = from_core.at[f, :, side]
                    add_into(landed, [src, landed])
            for k, f in enumerate(groups):
                begun.append(start(from_core.at[f], from_group.at[k], me.device(f=f)))
        elif number == 2:
            for side in range(2):
                add_into(
                    from_group.at[0, :, side],
                    [from_core.at[me.f, :, side]]
                    + [from_group.at[k, :, side] for k in range(fsdp - 1)],
                )
            begun.append(start(from_group.at[0, :, 1 - me.side], from_side, across))
        elif number == 3:
            add_into(from_side, [from_group.at[0, :, me.side], from_side])
            for k, rest in enumerate(others):
                begun.append(start(from_side.at[rest], from_rest.at[k], me.device(rest=rest)))
        elif number == 4:
            mine = out.at[(pl.ds(me.rest, 1), me.side, me.core) + window]
            add_into(
                mine,
                [from_side.at[pl.ds(me.rest, 1)]]
                + [from_rest.at[pl.ds(k, 1)] for k in range(rests - 1)],
            )
            for rest in others:
                begun.append(start(mine, mine, me.device(rest=rest)))
        elif number == 5:
            mine = out.at[(slice(None), me.side, me.core) + window]
            begun.append(start(mine, mine, across))
        elif number == 6:
            for side in range(2):
                mine = out.at[(slice(None), side, me.core) + window]
                begun.append(start(mine, mine, sibling))
        flying[i] = begun

    stages = 8
    for tick in range(stages + len(chunks) - 1):
        i = 0
        for c, chunk in enumerate(chunks):
            number = tick - c
            for part in chunk:
                if 0 <= number < stages:
                    stage(i, part, number)
                i += 1
    for copy in sent:
        copy.wait_send()


def reduce_everywhere(fsdp, replicas, grads, chunks):
    rests = replicas // 4
    count = len(grads)
    tails = [(part[2], part[4]) for chunk in chunks for part in chunk]
    copies = len(tails) * (2 * fsdp + (fsdp - 1) + 1 + (rests - 1) + (rests - 1) + 3)
    vmem = pl.BlockSpec(memory_space=pltpu.VMEM)
    return pl.pallas_call(
        functools.partial(reduce_kernel, fsdp, replicas, count, chunks),
        name="reduce_everywhere",
        in_specs=[vmem] * count,
        out_specs=[vmem] * count,
        out_shape=[
            jax.ShapeDtypeStruct((rests, 2, 2) + item.shape[-2:], bf16) for item in grads
        ],
        scratch_shapes=[pltpu.VMEM((fsdp, rests, 2) + tail, bf16) for tail in tails]
        + [pltpu.VMEM((fsdp - 1, rests, 2) + tail, bf16) for tail in tails]
        + [pltpu.VMEM((rests,) + tail, bf16) for tail in tails]
        + [pltpu.VMEM((rests - 1,) + tail, bf16) for tail in tails]
        + [pltpu.SemaphoreType.DMA((copies,))] * 2,
        compiler_params=pltpu.CompilerParams(
            collective_id=2, has_side_effects=True, vmem_limit_bytes=60 << 20
        ),
    )(*grads)


GELU_C = math.sqrt(2.0 / math.pi)


def gelu_both(v):
    square = v * v
    t = jnp.tanh(GELU_C * v * (1.0 + 0.044715 * square))
    half = 0.5 * (1.0 + t)
    slope = half + 0.5 * v * (1.0 - t * t) * GELU_C * (1.0 + 3 * 0.044715 * square)
    return v * half, slope


MLP_BLOCK = 512
MLP_ROWS = 512


def mlp_kernel(
    n_ref, nt_ref, g_ref, gt_ref, wi_ref, wo_ref, b_ref,
    y_ref, d_ref, gwi_ref, gwo_ref, gb_ref, act, dh,
):
    tokens, width = n_ref.shape

    @pl.when(pl.program_id(0) == 0)
    def _():
        y_ref[...] = jnp.zeros_like(y_ref)
        d_ref[...] = jnp.zeros_like(d_ref)

    gb_ref[...] = jnp.zeros_like(gb_ref)

    def first(i):
        at = pl.ds(pl.multiple_of(i * MLP_ROWS, MLP_ROWS), MLP_ROWS)
        return at, dot(n_ref[at, :], wi_ref[...]), dot_nt(g_ref[at, :], wo_ref[...])

    def rows(i, _):
        ahead = [first(i * 2)]
        for j in range(2):
            if j + 1 < 2:
                ahead.append(first(i * 2 + j + 1))
            at, hidden, pull = ahead[j]
            activated, slope = gelu_both(hidden + b_ref[...])
            activated = activated.astype(bf16)
            grad = (pull * slope).astype(bf16)
            act[at, :] = activated
            dh[at, :] = grad
            gb_ref[...] += jnp.sum(grad.astype(f32), axis=0, keepdims=True)
            y_ref[at, :] += dot(activated, wo_ref[...])
            d_ref[at, :] += dot_nt(grad, wi_ref[...])
        return 0

    lax.fori_loop(0, tokens // (MLP_ROWS * 2), rows, 0)
    for r in range(0, width, 256):
        at = slice(r, r + 256)
        gwi_ref[at, :] = dot(nt_ref[at, :], dh[...]).astype(bf16)
        gwo_ref[:, at] = dot(gt_ref[at, :], act[...]).astype(bf16).T


def mlp(normed, grad, w_in, w_out, b_in):
    tokens, width = normed.shape
    hidden = w_in.shape[1]
    steps = hidden // MLP_BLOCK
    once = pl.Buffered(1)
    tall = pl.BlockSpec((tokens, width), lambda i: (0, 0), pipeline_mode=once)
    flat = pl.BlockSpec((width, tokens), lambda i: (0, 0), pipeline_mode=once)
    into = pl.BlockSpec((width, MLP_BLOCK), lambda i: (0, i))
    out_of = pl.BlockSpec((MLP_BLOCK, width), lambda i: (i, 0))
    bias = pl.BlockSpec((1, MLP_BLOCK), lambda i: (0, i))
    return pl.pallas_call(
        mlp_kernel,
        name="mlp_both_ways",
        grid=(steps,),
        in_specs=[tall, flat, tall, flat, into, out_of, bias],
        out_specs=[tall, tall, into, out_of, bias],
        out_shape=[
            jax.ShapeDtypeStruct((tokens, width), f32),
            jax.ShapeDtypeStruct((tokens, width), f32),
            jax.ShapeDtypeStruct((width, hidden), bf16),
            jax.ShapeDtypeStruct((hidden, width), bf16),
            jax.ShapeDtypeStruct((1, hidden), f32),
        ],
        scratch_shapes=[pltpu.VMEM((tokens, MLP_BLOCK), bf16)] * 2,
        cost_estimate=pl.CostEstimate(
            flops=12 * tokens * width * hidden,
            bytes_accessed=tokens * width * 16,
            transcendentals=tokens * hidden,
        ),
        compiler_params=pltpu.CompilerParams(vmem_limit_bytes=58 << 20),
    )(normed, normed.T, grad, grad.T, w_in, w_out, b_in.reshape(1, hidden))


def on_device(fsdp, replicas, *args):
    (
        patches,
        ln_gain,
        ln_bias,
        w_qkv,
        b_qkv,
        qk_gain,
        w_proj,
        out_bias,
        w_in,
        b_in,
        w_out,
        lengths,
        cotangent,
    ) = args
    rows, slots, width = patches.shape
    tokens = rows * slots
    small = (ln_gain, ln_bias, b_qkv, qk_gain, out_bias, b_in)
    flat = jnp.concatenate([item.reshape(-1) for item in small])
    small_cols = -(-flat.shape[0] // (64 * PAIR)) * PAIR
    flat = jnp.pad(flat, (0, 64 * small_cols - flat.shape[0])).reshape(2, 2, 16, small_cols)
    shard_rows, columns = w_qkv.shape
    third = columns // 3
    w_qkv_full, flat_full, w_out_full = gather_quarters(
        fsdp,
        replicas,
        [w_qkv.reshape(2, 2, -1, columns), flat, w_out.reshape(2, 2, -1, width)],
        [
            [(0, third), (third, third), (2 * third, third)],
            [(0, small_cols)],
            [(0, width // 2), (width // 2, width // 2)],
        ],
    )
    w_qkv_full = w_qkv_full.reshape(width, columns)
    w_out_full = w_out_full.reshape(-1, width)
    flat_full, w_proj, w_in = lax.optimization_barrier((flat_full, w_proj, w_in))
    flat_full = flat_full.reshape(fsdp, -1).astype(f32)
    full_small = []
    at = 0
    for item in small:
        size = item.size
        piece = flat_full[:, at : at + size].reshape((fsdp,) + item.shape)
        at += size
        full_small.append(jnp.moveaxis(piece, 0, -2).reshape(item.shape[:-1] + (-1,)))
    gains, shifts, b_qkv_full, qk_gain_full, out_bias_full, b_in_full = full_small
    w_proj_full = lax.all_gather(w_proj, "fsdp", axis=0, tiled=True)
    w_in_full = lax.all_gather(w_in, "fsdp", axis=0, tiled=True)

    pic, inside, bounds = picture_tables(lengths, slots)
    pic = pic[:, :, None]
    pair_gain = jnp.concatenate([qk_gain_full, qk_gain_full], axis=1)
    inside = inside.reshape(tokens, 1)

    source = patches.reshape(tokens, width).astype(f32)
    n1, rstd1 = norm_stats(source)
    normed1 = (n1 * gains[0] + shifts[0]).astype(bf16)
    qkv = (dot(normed1, w_qkv_full) + b_qkv_full).astype(bf16).reshape(rows, slots, columns)
    attn, lse = attention(qkv, pic, bounds, pair_gain)
    attn_flat = attn.reshape(tokens, width)
    resid = source + dot(attn_flat, w_proj_full) + out_bias_full[0]
    n2, rstd2 = norm_stats(resid)
    normed2 = (n2 * gains[1] + shifts[1]).astype(bf16)
    grad_y = cotangent.reshape(tokens, width).astype(f32) * inside
    grad_mlp = grad_y.astype(bf16)

    branch, grad_norm2, grad_w_in, grad_w_out, grad_b_in = mlp(
        normed2, grad_mlp, w_in_full, w_out_full, b_in_full
    )
    grad_b_in = grad_b_in[0]
    block_out = (resid + branch + out_bias_full[1]).astype(bf16)
    tt = (((0,), (0,)), ((), ()))
    grad_bias_mlp = jnp.sum(grad_y, axis=0)
    back2, grad_gain2, grad_shift2 = norm_back(grad_norm2, n2, rstd2, gains[1])
    grad_resid = grad_y + back2
    grad_branch = grad_resid.astype(bf16)
    grad_bias_attn = jnp.sum(grad_branch.astype(f32), axis=0)
    grad_attn = dot_nt(grad_branch, w_proj_full).astype(bf16)
    grad_w_proj = lax.dot_general(attn_flat, grad_branch, tt, preferred_element_type=f32).astype(bf16)

    grad_qkv, stats = attention_back(
        qkv, attn, grad_attn.reshape(rows, slots, width), lse, pic, bounds, pair_gain
    )
    stats = jnp.sum(stats, axis=0)
    grad_qk_gain = jnp.sum(stats[0:2].reshape(2, H, HD), axis=1)
    grad_b_qkv = stats[2:5].reshape(-1)
    grad_qkv = grad_qkv.reshape(3, tokens, width)
    grad_w_qkv = [
        lax.dot_general(normed1, grad_qkv[i], tt, preferred_element_type=f32).astype(bf16)
        for i in range(3)
    ]
    grad_norm1 = sum(
        dot_nt(grad_qkv[i], w_qkv_full[:, i * width : (i + 1) * width]) for i in range(3)
    )
    back1, grad_gain1, grad_shift1 = norm_back(grad_norm1, n1, rstd1, gains[0])
    grad_patches = (grad_resid + back1).reshape(rows, slots, width)

    small_grads = (
        jnp.stack([grad_gain1, grad_gain2]),
        jnp.stack([grad_shift1, grad_shift2]),
        grad_b_qkv,
        grad_qk_gain,
        jnp.stack([grad_bias_attn, grad_bias_mlp]),
        grad_b_in,
    )
    flat_grads = jnp.concatenate(
        [
            jnp.moveaxis(item.reshape(item.shape[:-1] + (fsdp, -1)), -2, 0).reshape(fsdp, -1)
            for item in small_grads
        ],
        axis=1,
    ).astype(bf16)
    lead = (fsdp, replicas // 4, 2, 2)
    small_rows = 16
    flat_grads = jnp.pad(
        flat_grads, ((0, 0), (0, replicas * small_rows * PAIR - flat_grads.shape[1]))
    )
    payload = [grad_w_out, grad_w_in, *grad_w_qkv, grad_w_proj]
    payload = [item.reshape(lead + (-1, item.shape[-1])) for item in payload]
    payload.append(flat_grads.reshape(lead + (small_rows, PAIR)))
    whole = [(i, 0, item.shape[-2], 0, item.shape[-1]) for i, item in enumerate(payload)]
    out_half, in_half = whole[0][2] // 2, whole[1][4] // 2
    out_chunks = [[whole[0]]]
    if out_half % 16 == 0:
        out_chunks = [[(0, at, out_half, 0, width)] for at in (0, out_half)]
    in_chunks = [[(1, 0, whole[1][2], at, in_half)] for at in (0, in_half)]
    chunks = out_chunks + in_chunks + [[whole[2], whole[3]], [whole[4], whole[5], whole[6]]]
    reduced = reduce_everywhere(fsdp, replicas, payload, chunks)
    r_w_out, r_w_in, r_q, r_k, r_v, r_w_proj = (
        item.reshape(-1, item.shape[-1]) for item in reduced[:6]
    )
    r_w_qkv = jnp.concatenate([r_q, r_k, r_v], axis=1)
    r_flat = reduced[6].reshape(-1).astype(f32)
    r_small = []
    at = 0
    for item in small:
        r_small.append(r_flat[at : at + item.size].reshape(item.shape))
        at += item.size
    return (
        block_out.reshape(rows, slots, width),
        grad_patches,
        r_small[0],
        r_small[1],
        r_w_qkv.astype(f32),
        r_small[2],
        r_small[3],
        r_w_proj.astype(f32),
        r_small[4],
        r_w_in.astype(f32),
        r_small[5],
        r_w_out.astype(f32),
    )


def solution(mesh):
    fsdp = mesh.shape["fsdp"]
    replicas = mesh.shape["dp"]
    every = ("dp", "fsdp")
    by_row = P(every, None, None)
    last, lead = P(None, "fsdp"), P("fsdp", None)
    placed = (
        by_row,
        last,
        last,
        lead,
        P("fsdp"),
        last,
        lead,
        last,
        lead,
        P("fsdp"),
        lead,
        P(every, None),
        by_row,
    )
    outs = (by_row, by_row, last, last, lead, P("fsdp"), last, lead, last, lead, P("fsdp"), lead)
    return jax.shard_map(
        functools.partial(on_device, fsdp, replicas),
        mesh=mesh,
        in_specs=placed,
        out_specs=outs,
        check_vma=False,
    )
```

```python
import functools
import math

import jax
import jax.numpy as jnp
from jax import lax
from jax.experimental import pallas as pl
from jax.experimental.pallas import tpu as pltpu
from jax.sharding import PartitionSpec as P

H = 12
HD = 64
PAIR = 2 * HD
GROUP = 6
BLK = 256
MASK = 256.0
LOG2E = math.log2(math.e)
f32 = jnp.float32
bf16 = jnp.bfloat16
NT = (((1,), (1,)), ((), ()))


def dot(a, b):
    return jnp.dot(a, b, preferred_element_type=f32)


def dot_nt(a, b):
    return lax.dot_general(a, b, NT, preferred_element_type=f32)


def lanes(rows):
    return lax.broadcasted_iota(jnp.int32, (rows, PAIR), 1)


def half_matrix(same, value):
    i = lax.broadcasted_iota(jnp.int32, (PAIR, PAIR), 0) // HD
    j = lax.broadcasted_iota(jnp.int32, (PAIR, PAIR), 1) // HD
    hit = (i == j) if same else (i != j)
    return jnp.where(hit, value, 0.0).astype(bf16)


def head_stats(raws, averager):
    means = [dot(raw, averager) for raw in raws]
    centered = [raw.astype(f32) - mean for raw, mean in zip(raws, means)]
    variances = [dot((item * item).astype(bf16), averager) for item in centered]
    rstds = [lax.rsqrt(item + 1e-6) for item in variances]
    return [item * rstd for item, rstd in zip(centered, rstds)], rstds


def split(v):
    high = v.astype(bf16)
    low = (v - high.astype(f32)).astype(bf16)
    return high, low


def query_extra(pic, lane):
    slot = lane % HD
    hot = jnp.where(slot == pic, MASK, 0.0)
    return jnp.where(slot == 11, -MASK, hot)


def key_extra(pic, lane):
    slot = lane % HD
    hot = jnp.where(slot == pic, 1.0, 0.0)
    return jnp.where(slot == 11, 1.0, jnp.where((slot == 12) | (slot == 13), -1.0, hot))


def forward_kernel(
    bounds, q_ref, k_ref, v_ref, pic_ref, gain_ref, out_ref, lse_ref, qa, ka, va, acc
):
    row = pl.program_id(0)
    slots = q_ref.shape[1]
    blocks = slots // BLK
    averager = half_matrix(True, 1.0 / HD)
    lane = lanes(BLK)
    low_half = lane < HD
    heads = 2 * GROUP

    def prepare(b, _):
        at = pl.ds(pl.multiple_of(b * BLK, BLK), BLK)
        pic = pic_ref[0, at, :]
        q_more = query_extra(pic, lane)
        k_more = key_extra(pic, lane)
        cols = [slice(p * PAIR, (p + 1) * PAIR) for p in range(GROUP)]
        raws = [q_ref[0, at, col] for col in cols] + [k_ref[0, at, col] for col in cols]
        normed, _unused = head_stats(raws, averager)
        for p, col in enumerate(cols):
            q = (normed[p] * gain_ref[0:1, :]).astype(bf16).astype(f32) * 0.125
            k = normed[GROUP + p] * gain_ref[1:2, :]
            v = v_ref[0, at, col].astype(f32)
            qa[2 * p, at, :] = jnp.where(low_half, q, q_more).astype(bf16)
            qa[2 * p + 1, at, :] = jnp.where(low_half, q_more, q).astype(bf16)
            ka[2 * p, at, :] = jnp.where(low_half, k, k_more).astype(bf16)
            ka[2 * p + 1, at, :] = jnp.where(low_half, k_more, k).astype(bf16)
            va[2 * p, at, :] = jnp.where(low_half, v, 1.0).astype(bf16)
            va[2 * p + 1, at, :] = jnp.where(low_half, 1.0, v).astype(bf16)
        return 0

    lax.fori_loop(0, blocks, prepare, 0)

    def query_block(b, _):
        at = pl.ds(pl.multiple_of(b * BLK, BLK), BLK)
        acc[...] = jnp.zeros_like(acc)

        def key_block(kb, _):
            keys = pl.ds(pl.multiple_of(kb * BLK, BLK), BLK)
            ahead = [dot_nt(qa[0, at, :], ka[0, keys, :])]
            for h in range(heads):
                if h + 1 < heads:
                    ahead.append(dot_nt(qa[h + 1, at, :], ka[h + 1, keys, :]))
                probs = jnp.exp2(ahead[h] * LOG2E).astype(bf16)
                acc[h] += dot(probs, va[h, keys, :])
            return 0

        lax.fori_loop(bounds[row, 0, b], bounds[row, 1, b], key_block, 0)
        for p in range(GROUP):
            col = slice(p * PAIR, (p + 1) * PAIR)
            even, odd = acc[2 * p], acc[2 * p + 1]
            crossed = jnp.where(low_half, odd, even)
            total = pltpu.roll(crossed, HD, 1)
            out_ref[0, at, col] = (jnp.where(low_half, even, odd) / total).astype(bf16)
            lse_ref[0, at, col] = jnp.log(crossed)
        return 0

    lax.fori_loop(0, blocks, query_block, 0)


def backward_kernel(
    bounds,
    q_ref,
    k_ref,
    v_ref,
    o_ref,
    g_ref,
    lse_ref,
    pic_ref,
    gain_ref,
    out_q,
    out_k,
    out_v,
    stat_ref,
    qa,
    ka,
    va,
    ga,
    kt,
    dqt,
    dk,
    dv,
):
    row = pl.program_id(0)
    slots = q_ref.shape[1]
    blocks = slots // BLK
    averager = half_matrix(True, 1.0 / HD)
    crosser = half_matrix(False, 1.0)
    lane = lanes(BLK)
    slot = lane % HD
    low_half = lane < HD
    heads = 2 * GROUP

    def prepare(b, _):
        at = pl.ds(pl.multiple_of(b * BLK, BLK), BLK)
        pic = pic_ref[0, at, :]
        q_hot = query_extra(pic, lane)
        k_more = key_extra(pic, lane)
        cols = [slice(p * PAIR, (p + 1) * PAIR) for p in range(GROUP)]
        raws = [q_ref[0, at, col] for col in cols] + [k_ref[0, at, col] for col in cols]
        normed, _unused = head_stats(raws, averager)
        grads = [g_ref[0, at, col].astype(f32) for col in cols]
        parts = [split(g * o_ref[0, at, col].astype(f32)) for g, col in zip(grads, cols)]
        centres = [dot(high, crosser) + dot(low, crosser) for high, low in parts]
        for p, col in enumerate(cols):
            lse = lse_ref[0, at, col]
            lse_high = lse.astype(bf16).astype(f32)
            q_more = jnp.where(slot == 12, lse_high, jnp.where(slot == 13, lse - lse_high, q_hot))
            q = (normed[p] * gain_ref[0:1, :]).astype(bf16).astype(f32) * 0.125
            k = normed[GROUP + p] * gain_ref[1:2, :]
            v = v_ref[0, at, col].astype(f32)
            g, centre = grads[p], centres[p]
            centre_high = centre.astype(bf16).astype(f32)
            g_more = jnp.where(
                slot == 12, centre_high, jnp.where(slot == 13, centre - centre_high, 0.0)
            )
            v_more = jnp.where((slot == 12) | (slot == 13), -1.0, 0.0)
            qa[2 * p, at, :] = jnp.where(low_half, q, q_more).astype(bf16)
            qa[2 * p + 1, at, :] = jnp.where(low_half, q_more, q).astype(bf16)
            ka[2 * p, at, :] = jnp.where(low_half, k, k_more).astype(bf16)
            ka[2 * p + 1, at, :] = jnp.where(low_half, k_more, k).astype(bf16)
            va[2 * p, at, :] = jnp.where(low_half, v, v_more).astype(bf16)
            va[2 * p + 1, at, :] = jnp.where(low_half, v_more, v).astype(bf16)
            ga[2 * p, at, :] = jnp.where(low_half, g, g_more).astype(bf16)
            ga[2 * p + 1, at, :] = jnp.where(low_half, g_more, g).astype(bf16)
            kt[p, :, at] = k.astype(bf16).T
        return 0

    lax.fori_loop(0, blocks, prepare, 0)
    dqt[...] = jnp.zeros_like(dqt)
    stat_ref[...] = jnp.zeros_like(stat_ref)

    cols = [slice(p * PAIR, (p + 1) * PAIR) for p in range(GROUP)]

    def pull_norm(raws, grads, gain):
        normed, rstds = head_stats(raws, averager)
        lifted = [grad * gain for grad in grads]
        ones = [dot(item.astype(bf16), averager) for item in lifted]
        twos = [dot((a * n).astype(bf16), averager) for a, n in zip(lifted, normed)]
        raw_grads = [
            (rstd * (a - one - n * two)).astype(bf16)
            for rstd, a, one, n, two in zip(rstds, lifted, ones, normed, twos)
        ]
        return raw_grads, [
            jnp.sum(grad * n, axis=0, keepdims=True) for grad, n in zip(grads, normed)
        ]

    def key_block(b, _):
        keys = pl.ds(pl.multiple_of(b * BLK, BLK), BLK)
        dk[...] = jnp.zeros_like(dk)
        dv[...] = jnp.zeros_like(dv)

        def query_block(qb, _):
            at = pl.ds(pl.multiple_of(qb * BLK, BLK), BLK)
            def first(h):
                return (
                    dot_nt(ka[h, keys, :], qa[h, at, :]),
                    dot_nt(va[h, keys, :], ga[h, at, :]),
                )

            ahead = [first(0)]
            for h in range(heads):
                p, half = h // 2, slice((h % 2) * HD, (h % 2 + 1) * HD)
                if h + 1 < heads:
                    ahead.append(first(h + 1))
                scores, pulls = ahead[h]
                probs = jnp.exp2(scores * LOG2E)
                grads = (probs * pulls).astype(bf16)
                dv[h] += dot(probs.astype(bf16), ga[h, at, :])
                dk[h] += dot(grads, qa[h, at, :])
                dqt[p, half, at] += dot(kt[p, half, keys], grads)
            return 0

        lax.fori_loop(bounds[row, 2, b], bounds[row, 3, b], query_block, 0)
        grads = [jnp.where(low_half, dk[2 * p], dk[2 * p + 1]) for p in range(GROUP)]
        raw_grads, gain_grads = pull_norm(
            [k_ref[0, keys, col] for col in cols], grads, gain_ref[1:2, :]
        )
        for p, col in enumerate(cols):
            raw_grad = raw_grads[p]
            out_k[0, keys, col] = raw_grad
            stat_ref[0, 1:2, col] += gain_grads[p]
            stat_ref[0, 3:4, col] += jnp.sum(raw_grad.astype(f32), axis=0, keepdims=True)
            grad_v = jnp.where(low_half, dv[2 * p], dv[2 * p + 1]).astype(bf16)
            out_v[0, keys, col] = grad_v
            stat_ref[0, 4:5, col] += jnp.sum(grad_v.astype(f32), axis=0, keepdims=True)
        return 0

    lax.fori_loop(0, blocks, key_block, 0)

    def finish(b, _):
        at = pl.ds(pl.multiple_of(b * BLK, BLK), BLK)
        grads = [dqt[p, :, at].T * 0.125 for p in range(GROUP)]
        raw_grads, gain_grads = pull_norm(
            [q_ref[0, at, col] for col in cols], grads, gain_ref[0:1, :]
        )
        for p, col in enumerate(cols):
            raw_grad = raw_grads[p]
            out_q[0, at, col] = raw_grad
            stat_ref[0, 0:1, col] += gain_grads[p]
            stat_ref[0, 2:3, col] += jnp.sum(raw_grad.astype(f32), axis=0, keepdims=True)
        return 0

    lax.fori_loop(0, blocks, finish, 0)


def attention(qkv, pic, bounds, gains):
    rows, slots, _ = qkv.shape
    width = qkv.shape[2] // 3
    wide = GROUP * PAIR
    groups = width // wide
    flops = rows * H * slots * slots * 256 * 4
    part = lambda i: pl.BlockSpec((1, slots, wide), lambda r, g, b: (r, 0, i * groups + g))
    whole = pl.BlockSpec((1, slots, wide), lambda r, g, b: (r, 0, g))
    return pl.pallas_call(
        forward_kernel,
        name="attention_forward",
        grid_spec=pltpu.PrefetchScalarGridSpec(
            num_scalar_prefetch=1,
            grid=(rows, groups),
            in_specs=[
                part(0),
                part(1),
                part(2),
                pl.BlockSpec((1, slots, 1), lambda r, g, b: (r, 0, 0)),
                pl.BlockSpec((2, PAIR), lambda r, g, b: (0, 0)),
            ],
            out_specs=[whole, whole],
            scratch_shapes=[
                pltpu.VMEM((2 * GROUP, slots, PAIR), bf16),
                pltpu.VMEM((2 * GROUP, slots, PAIR), bf16),
                pltpu.VMEM((2 * GROUP, slots, PAIR), bf16),
                pltpu.VMEM((2 * GROUP, BLK, PAIR), f32),
            ],
        ),
        out_shape=[
            jax.ShapeDtypeStruct((rows, slots, width), bf16),
            jax.ShapeDtypeStruct((rows, slots, width), f32),
        ],
        cost_estimate=pl.CostEstimate(
            flops=flops, bytes_accessed=rows * slots * width * 12, transcendentals=0
        ),
        compiler_params=pltpu.CompilerParams(vmem_limit_bytes=48 << 20),
    )(bounds, qkv, qkv, qkv, pic, gains)


def attention_back(qkv, attn, grad_attn, lse, pic, bounds, gains):
    rows, slots, _ = qkv.shape
    width = qkv.shape[2] // 3
    wide = GROUP * PAIR
    groups = width // wide
    flops = rows * H * slots * slots * 256 * 10
    part = lambda i: pl.BlockSpec((1, slots, wide), lambda r, g, b: (r, 0, i * groups + g))
    whole = pl.BlockSpec((1, slots, wide), lambda r, g, b: (r, 0, g))
    return pl.pallas_call(
        backward_kernel,
        name="attention_backward",
        grid_spec=pltpu.PrefetchScalarGridSpec(
            num_scalar_prefetch=1,
            grid=(rows, groups),
            in_specs=[
                part(0),
                part(1),
                part(2),
                whole,
                whole,
                whole,
                pl.BlockSpec((1, slots, 1), lambda r, g, b: (r, 0, 0)),
                pl.BlockSpec((2, PAIR), lambda r, g, b: (0, 0)),
            ],
            out_specs=[
                whole,
                whole,
                whole,
                pl.BlockSpec((1, 8, wide), lambda r, g, b: (r, 0, g)),
            ],
            scratch_shapes=[
                pltpu.VMEM((2 * GROUP, slots, PAIR), bf16),
                pltpu.VMEM((2 * GROUP, slots, PAIR), bf16),
                pltpu.VMEM((2 * GROUP, slots, PAIR), bf16),
                pltpu.VMEM((2 * GROUP, slots, PAIR), bf16),
                pltpu.VMEM((GROUP, PAIR, slots), bf16),
                pltpu.VMEM((GROUP, PAIR, slots), f32),
                pltpu.VMEM((2 * GROUP, BLK, PAIR), f32),
                pltpu.VMEM((2 * GROUP, BLK, PAIR), f32),
            ],
        ),
        out_shape=[
            jax.ShapeDtypeStruct((rows, slots, width), bf16),
            jax.ShapeDtypeStruct((rows, slots, width), bf16),
            jax.ShapeDtypeStruct((rows, slots, width), bf16),
            jax.ShapeDtypeStruct((rows, 8, width), f32),
        ],
        cost_estimate=pl.CostEstimate(
            flops=flops, bytes_accessed=rows * slots * width * 20, transcendentals=0
        ),
        compiler_params=pltpu.CompilerParams(vmem_limit_bytes=56 << 20),
    )(bounds, qkv, qkv, qkv, attn, grad_attn, lse, pic, gains)


def picture_tables(lengths, slots):
    ends = jnp.cumsum(lengths, axis=1)
    position = jnp.arange(slots, dtype=jnp.int32)
    pic = jnp.sum((position[None, :, None] >= ends[:, None, :]).astype(jnp.int32), axis=2)
    inside = (position[None, :] < ends[:, -1:]).astype(f32)
    first = jnp.arange(0, slots, BLK, dtype=jnp.int32)
    last = first + (BLK - 1)
    before = jnp.where(ends[:, None, :] <= first[None, :, None], ends[:, None, :], 0)
    begin = jnp.max(before, axis=2)
    after = jnp.where(ends[:, None, :] > last[None, :, None], ends[:, None, :], slots)
    end = jnp.min(after, axis=2)
    low = begin // BLK
    high = (end + BLK - 1) // BLK
    used = ((ends[:, -1:] + BLK - 1) // BLK) * jnp.ones_like(high)
    index = jnp.arange(slots // BLK, dtype=jnp.int32)[None, :]
    low_back = low
    high_back = jnp.where(index < used, jnp.minimum(high, used), low)
    bounds = jnp.stack([low, high, low_back, high_back], axis=1).astype(jnp.int32)
    return pic.astype(jnp.int32), inside, bounds


def norm_stats(values):
    mean = jnp.mean(values, axis=-1, keepdims=True)
    centered = values - mean
    variance = jnp.mean(centered * centered, axis=-1, keepdims=True)
    rstd = lax.rsqrt(variance + 1e-6)
    return centered * rstd, rstd


def norm_back(grad, normed, rstd, gain):
    lifted = grad * gain
    mean_one = jnp.mean(lifted, axis=-1, keepdims=True)
    mean_two = jnp.mean(lifted * normed, axis=-1, keepdims=True)
    return (
        rstd * (lifted - mean_one - normed * mean_two),
        jnp.sum(grad * normed, axis=0),
        jnp.sum(grad, axis=0),
    )


class Place:
    def __init__(self, fsdp, replicas):
        self.groups, self.rests = fsdp, replicas // 4
        dp = lax.axis_index("dp")
        self.f = lax.axis_index("fsdp")
        self.core = lax.rem(dp, 2)
        self.side = lax.rem(dp // 2, 2)
        self.rest = dp // 4

    def device(self, f=None, core=None, side=None, rest=None):
        f = self.f if f is None else f
        core = self.core if core is None else core
        side = self.side if side is None else side
        rest = self.rest if rest is None else rest
        return ((rest * 2 + side) * 2 + core, f)


def remote(src, dst, send, recv, device):
    return pltpu.make_async_remote_copy(
        src_ref=src,
        dst_ref=dst,
        send_sem=send,
        recv_sem=recv,
        device_id=device,
        device_id_type=pl.DeviceIdType.MESH,
    )


def greet(devices):
    barrier = pltpu.get_barrier_semaphore()
    for device in devices:
        pl.semaphore_signal(
            barrier, inc=1, device_id=device, device_id_type=pl.DeviceIdType.MESH
        )
    pl.semaphore_wait(barrier, len(devices))


def gather_kernel(fsdp, replicas, pieces, *refs):
    count = len(pieces)
    shards, fulls = refs[:count], refs[count : 2 * count]
    own_sem, sends, recvs = refs[2 * count :]
    me = Place(fsdp, replicas)
    sibling = me.device(core=1 - me.core)
    across = me.device(side=1 - me.side)
    peers = [lax.rem(me.f + k, fsdp) for k in range(1, fsdp)]
    sources = [lax.rem(me.f + fsdp - k, fsdp) for k in range(1, fsdp)]
    greet([sibling, across] + [me.device(f=peer) for peer in peers])
    outer, crossing, inner = [], [], []
    for i in range(count):
        for start, size in pieces[i]:
            col = pl.ds(start, size)
            for k, peer in enumerate(peers):
                at = len(outer)
                copy = remote(
                    shards[i].at[me.side, me.core, :, col],
                    fulls[i].at[me.f, me.side, me.core, :, col],
                    sends.at[0, at],
                    recvs.at[0, at],
                    me.device(f=peer),
                )
                copy.start()
                outer.append((copy, i, col, k))
    own = []
    for i in range(count):
        copy = pltpu.make_async_copy(shards[i], fulls[i].at[me.f], own_sem.at[i])
        copy.start()
        own.append(copy)

    def forward(landed, kind, at, device):
        copy = remote(landed, landed, sends.at[kind, at], recvs.at[kind, at], device)
        copy.start()
        return copy

    for at in range(len(outer) + 1):
        if at < len(outer):
            copy, i, col, k = outer[at]
            copy.wait_recv()
            landed = fulls[i].at[sources[k], me.side, me.core, :, col]
            crossing.append(forward(landed, 1, at, across))
            inner.append(forward(landed, 2, at, sibling))
        if at > 0:
            _unused, i, col, k = outer[at - 1]
            crossing[at - 1].wait_recv()
            landed = fulls[i].at[sources[k], 1 - me.side, me.core, :, col]
            inner.append(forward(landed, 3, at - 1, sibling))
    for copy, *_unused in outer:
        copy.wait_send()
    for copy in crossing:
        copy.wait_send()
    for copy in inner:
        copy.wait()
    for copy in own:
        copy.wait()


def gather_quarters(fsdp, replicas, shards, pieces):
    copies = sum(len(item) for item in pieces) * (fsdp - 1)
    vmem = pl.BlockSpec(memory_space=pltpu.VMEM)
    return pl.pallas_call(
        functools.partial(gather_kernel, fsdp, replicas, pieces),
        name="gather_quarters",
        in_specs=[vmem] * len(shards),
        out_specs=[vmem] * len(shards),
        out_shape=[jax.ShapeDtypeStruct((fsdp,) + item.shape, item.dtype) for item in shards],
        scratch_shapes=[pltpu.SemaphoreType.DMA((len(shards),))]
        + [pltpu.SemaphoreType.DMA((4, copies))] * 2,
        compiler_params=pltpu.CompilerParams(
            collective_id=1, has_side_effects=True, vmem_limit_bytes=32 << 20
        ),
    )(*shards)


def add_into(dst, sources):
    def step(i, _):
        total = sources[0][i].astype(f32)
        for item in sources[1:]:
            total = total + item[i].astype(f32)
        dst[i] = total.astype(bf16)
        return 0

    lax.fori_loop(0, dst.shape[0], step, 0)


def reduce_kernel(fsdp, replicas, count, chunks, *refs):
    grads, outs = refs[:count], refs[count : 2 * count]
    parts = sum(len(chunk) for chunk in chunks)
    buffers = refs[2 * count : -2]
    send, recv = refs[-2:]
    me = Place(fsdp, replicas)
    rests = replicas // 4
    sibling = me.device(core=1 - me.core)
    across = me.device(side=1 - me.side)
    groups = [lax.rem(me.f + k, fsdp) for k in range(1, fsdp)]
    others = [lax.rem(me.rest + k, rests) for k in range(1, rests)]
    greet(
        [sibling, across]
        + [me.device(f=item) for item in groups]
        + [me.device(rest=item) for item in others]
    )
    used = [0]

    def start(src, dst, device):
        at = used[0]
        used[0] += 1
        copy = remote(src, dst, send.at[at], recv.at[at], device)
        copy.start()
        return copy

    sent = []
    flying = [None] * parts

    def stage(i, part, number):
        array, row, rows, col, cols = part
        window = (pl.ds(row, rows), pl.ds(col, cols))
        grad, out = grads[array], outs[array]
        from_core, from_group, from_side, from_rest = (
            buffers[i],
            buffers[parts + i],
            buffers[2 * parts + i],
            buffers[3 * parts + i],
        )
        if number > 0:
            for copy in flying[i]:
                copy.wait_recv()
                sent.append(copy)
        begun = []
        if number == 0:
            for f in range(fsdp):
                for side in range(2):
                    src = grad.at[(f, slice(None), side, 1 - me.core) + window]
                    begun.append(start(src, from_core.at[f, :, side], sibling))
        elif number == 1:
            for f in range(fsdp):
                for side in range(2):
                    src = grad.at[(f, slice(None), side, me.core) + window]
                    landed = from_core.at[f, :, side]
                    add_into(landed, [src, landed])
            for k, f in enumerate(groups):
                begun.append(start(from_core.at[f], from_group.at[k], me.device(f=f)))
        elif number == 2:
            for side in range(2):
                add_into(
                    from_group.at[0, :, side],
                    [from_core.at[me.f, :, side]]
                    + [from_group.at[k, :, side] for k in range(fsdp - 1)],
                )
            begun.append(start(from_group.at[0, :, 1 - me.side], from_side, across))
        elif number == 3:
            add_into(from_side, [from_group.at[0, :, me.side], from_side])
            for k, rest in enumerate(others):
                begun.append(start(from_side.at[rest], from_rest.at[k], me.device(rest=rest)))
        elif number == 4:
            mine = out.at[(pl.ds(me.rest, 1), me.side, me.core) + window]
            add_into(
                mine,
                [from_side.at[pl.ds(me.rest, 1)]]
                + [from_rest.at[pl.ds(k, 1)] for k in range(rests - 1)],
            )
            for rest in others:
                begun.append(start(mine, mine, me.device(rest=rest)))
        elif number == 5:
            mine = out.at[(slice(None), me.side, me.core) + window]
            begun.append(start(mine, mine, across))
        elif number == 6:
            for side in range(2):
                mine = out.at[(slice(None), side, me.core) + window]
                begun.append(start(mine, mine, sibling))
        flying[i] = begun

    stages = 8
    for tick in range(stages + len(chunks) - 1):
        i = 0
        for c, chunk in enumerate(chunks):
            number = tick - c
            for part in chunk:
                if 0 <= number < stages:
                    stage(i, part, number)
                i += 1
    for copy in sent:
        copy.wait_send()


def reduce_everywhere(fsdp, replicas, grads, chunks):
    rests = replicas // 4
    count = len(grads)
    tails = [(part[2], part[4]) for chunk in chunks for part in chunk]
    copies = len(tails) * (2 * fsdp + (fsdp - 1) + 1 + (rests - 1) + (rests - 1) + 3)
    vmem = pl.BlockSpec(memory_space=pltpu.VMEM)
    return pl.pallas_call(
        functools.partial(reduce_kernel, fsdp, replicas, count, chunks),
        name="reduce_everywhere",
        in_specs=[vmem] * count,
        out_specs=[vmem] * count,
        out_shape=[
            jax.ShapeDtypeStruct((rests, 2, 2) + item.shape[-2:], bf16) for item in grads
        ],
        scratch_shapes=[pltpu.VMEM((fsdp, rests, 2) + tail, bf16) for tail in tails]
        + [pltpu.VMEM((fsdp - 1, rests, 2) + tail, bf16) for tail in tails]
        + [pltpu.VMEM((rests,) + tail, bf16) for tail in tails]
        + [pltpu.VMEM((rests - 1,) + tail, bf16) for tail in tails]
        + [pltpu.SemaphoreType.DMA((copies,))] * 2,
        compiler_params=pltpu.CompilerParams(
            collective_id=2, has_side_effects=True, vmem_limit_bytes=60 << 20
        ),
    )(*grads)


GELU_C = math.sqrt(2.0 / math.pi)


def gelu_both(v):
    square = v * v
    t = jnp.tanh(GELU_C * v * (1.0 + 0.044715 * square))
    half = 0.5 * (1.0 + t)
    slope = half + 0.5 * v * (1.0 - t * t) * GELU_C * (1.0 + 3 * 0.044715 * square)
    return v * half, slope


MLP_BLOCK = 512
MLP_ROWS = 512


def mlp_kernel(
    n_ref, g_ref, wi_ref, wo_ref, b_ref,
    y_ref, d_ref, gwi_ref, gwo_ref, gb_ref, act, dh, nt, gt,
):
    tokens, width = n_ref.shape

    @pl.when(pl.program_id(0) == 0)
    def _():
        y_ref[...] = jnp.zeros_like(y_ref)
        d_ref[...] = jnp.zeros_like(d_ref)

        def turn(i, _):
            at = pl.ds(pl.multiple_of(i * 256, 256), 256)
            nt[:, at] = n_ref[at, :].T
            gt[:, at] = g_ref[at, :].T
            return 0

        lax.fori_loop(0, tokens // 256, turn, 0)

    gb_ref[...] = jnp.zeros_like(gb_ref)

    def first(i):
        at = pl.ds(pl.multiple_of(i * MLP_ROWS, MLP_ROWS), MLP_ROWS)
        return at, dot(n_ref[at, :], wi_ref[...]), dot_nt(g_ref[at, :], wo_ref[...])

    def rows(i, _):
        ahead = [first(i * 2)]
        for j in range(2):
            if j + 1 < 2:
                ahead.append(first(i * 2 + j + 1))
            at, hidden, pull = ahead[j]
            activated, slope = gelu_both(hidden + b_ref[...])
            activated = activated.astype(bf16)
            grad = (pull * slope).astype(bf16)
            act[at, :] = activated
            dh[at, :] = grad
            gb_ref[...] += jnp.sum(grad.astype(f32), axis=0, keepdims=True)
            y_ref[at, :] += dot(activated, wo_ref[...])
            d_ref[at, :] += dot_nt(grad, wi_ref[...])
        return 0

    lax.fori_loop(0, tokens // (MLP_ROWS * 2), rows, 0)
    for r in range(0, width, 256):
        at = slice(r, r + 256)
        gwi_ref[at, :] = dot(nt[at, :], dh[...]).astype(bf16)
        gwo_ref[:, at] = dot(gt[at, :], act[...]).astype(bf16).T


def mlp(normed, grad, w_in, w_out, b_in):
    tokens, width = normed.shape
    hidden = w_in.shape[1]
    steps = hidden // MLP_BLOCK
    once = pl.Buffered(1)
    tall = pl.BlockSpec((tokens, width), lambda i: (0, 0), pipeline_mode=once)
    into = pl.BlockSpec((width, MLP_BLOCK), lambda i: (0, i))
    out_of = pl.BlockSpec((MLP_BLOCK, width), lambda i: (i, 0))
    bias = pl.BlockSpec((1, MLP_BLOCK), lambda i: (0, i))
    return pl.pallas_call(
        mlp_kernel,
        name="mlp_both_ways",
        grid=(steps,),
        in_specs=[tall, tall, into, out_of, bias],
        out_specs=[tall, tall, into, out_of, bias],
        out_shape=[
            jax.ShapeDtypeStruct((tokens, width), f32),
            jax.ShapeDtypeStruct((tokens, width), f32),
            jax.ShapeDtypeStruct((width, hidden), bf16),
            jax.ShapeDtypeStruct((hidden, width), bf16),
            jax.ShapeDtypeStruct((1, hidden), f32),
        ],
        scratch_shapes=[pltpu.VMEM((tokens, MLP_BLOCK), bf16)] * 2
        + [pltpu.VMEM((width, tokens), bf16)] * 2,
        cost_estimate=pl.CostEstimate(
            flops=12 * tokens * width * hidden,
            bytes_accessed=tokens * width * 16,
            transcendentals=tokens * hidden,
        ),
        compiler_params=pltpu.CompilerParams(vmem_limit_bytes=58 << 20),
    )(normed, grad, w_in, w_out, b_in.reshape(1, hidden))


def on_device(fsdp, replicas, *args):
    (
        patches,
        ln_gain,
        ln_bias,
        w_qkv,
        b_qkv,
        qk_gain,
        w_proj,
        out_bias,
        w_in,
        b_in,
        w_out,
        lengths,
        cotangent,
    ) = args
    rows, slots, width = patches.shape
    tokens = rows * slots
    small = (ln_gain, ln_bias, b_qkv, qk_gain, out_bias, b_in)
    flat = jnp.concatenate([item.reshape(-1) for item in small])
    small_cols = -(-flat.shape[0] // (64 * PAIR)) * PAIR
    flat = jnp.pad(flat, (0, 64 * small_cols - flat.shape[0])).reshape(2, 2, 16, small_cols)
    shard_rows, columns = w_qkv.shape
    third = columns // 3
    w_qkv_full, flat_full, w_out_full = gather_quarters(
        fsdp,
        replicas,
        [w_qkv.reshape(2, 2, -1, columns), flat, w_out.reshape(2, 2, -1, width)],
        [
            [(0, third), (third, third), (2 * third, third)],
            [(0, small_cols)],
            [(0, width // 2), (width // 2, width // 2)],
        ],
    )
    w_qkv_full = w_qkv_full.reshape(width, columns)
    w_out_full = w_out_full.reshape(-1, width)
    flat_full, w_proj, w_in = lax.optimization_barrier((flat_full, w_proj, w_in))
    flat_full = flat_full.reshape(fsdp, -1).astype(f32)
    full_small = []
    at = 0
    for item in small:
        size = item.size
        piece = flat_full[:, at : at + size].reshape((fsdp,) + item.shape)
        at += size
        full_small.append(jnp.moveaxis(piece, 0, -2).reshape(item.shape[:-1] + (-1,)))
    gains, shifts, b_qkv_full, qk_gain_full, out_bias_full, b_in_full = full_small
    w_proj_full = lax.all_gather(w_proj, "fsdp", axis=0, tiled=True)
    w_in_full = lax.all_gather(w_in, "fsdp", axis=0, tiled=True)

    pic, inside, bounds = picture_tables(lengths, slots)
    pic = pic[:, :, None]
    pair_gain = jnp.concatenate([qk_gain_full, qk_gain_full], axis=1)
    inside = inside.reshape(tokens, 1)

    source = patches.reshape(tokens, width).astype(f32)
    n1, rstd1 = norm_stats(source)
    normed1 = (n1 * gains[0] + shifts[0]).astype(bf16)
    qkv = (dot(normed1, w_qkv_full) + b_qkv_full).astype(bf16).reshape(rows, slots, columns)
    attn, lse = attention(qkv, pic, bounds, pair_gain)
    attn_flat = attn.reshape(tokens, width)
    resid = source + dot(attn_flat, w_proj_full) + out_bias_full[0]
    n2, rstd2 = norm_stats(resid)
    normed2 = (n2 * gains[1] + shifts[1]).astype(bf16)
    grad_y = cotangent.reshape(tokens, width).astype(f32) * inside
    grad_mlp = grad_y.astype(bf16)

    branch, grad_norm2, grad_w_in, grad_w_out, grad_b_in = mlp(
        normed2, grad_mlp, w_in_full, w_out_full, b_in_full
    )
    grad_b_in = grad_b_in[0]
    block_out = (resid + branch + out_bias_full[1]).astype(bf16)
    tt = (((0,), (0,)), ((), ()))
    grad_bias_mlp = jnp.sum(grad_y, axis=0)
    back2, grad_gain2, grad_shift2 = norm_back(grad_norm2, n2, rstd2, gains[1])
    grad_resid = grad_y + back2
    grad_branch = grad_resid.astype(bf16)
    grad_bias_attn = jnp.sum(grad_branch.astype(f32), axis=0)
    grad_attn = dot_nt(grad_branch, w_proj_full).astype(bf16)
    grad_w_proj = lax.dot_general(attn_flat, grad_branch, tt, preferred_element_type=f32).astype(bf16)

    *grad_qkv, stats = attention_back(
        qkv, attn, grad_attn.reshape(rows, slots, width), lse, pic, bounds, pair_gain
    )
    stats = jnp.sum(stats, axis=0)
    grad_qkv = [item.reshape(tokens, width) for item in grad_qkv]
    grad_w_qkv = [
        lax.dot_general(normed1, grad_qkv[i], tt, preferred_element_type=f32).astype(bf16)
        for i in range(3)
    ]
    grad_norm1 = sum(
        dot_nt(grad_qkv[i], w_qkv_full[:, i * width : (i + 1) * width]) for i in range(3)
    )
    back1, grad_gain1, grad_shift1 = norm_back(grad_norm1, n1, rstd1, gains[0])
    grad_patches = (grad_resid + back1).reshape(rows, slots, width)

    lead = (fsdp, replicas // 4, 2, 2)
    small_rows = [
        stats[0:5],
        jnp.stack([grad_gain1, grad_gain2, grad_shift1, grad_shift2]),
        jnp.stack([grad_bias_attn, grad_bias_mlp]),
        grad_b_in.reshape(-1, width),
    ]
    small_rows = jnp.concatenate(small_rows, axis=0).astype(bf16)
    row_count = small_rows.shape[0]
    per_device = -(-row_count // replicas)
    small_rows = jnp.pad(small_rows, ((0, replicas * per_device - row_count), (0, 0)))
    small_rows = jnp.broadcast_to(
        small_rows.reshape(lead[1:] + (per_device, width)), lead + (per_device, width)
    )
    payload = [grad_w_out, grad_w_in, *grad_w_qkv, grad_w_proj]
    payload = [item.reshape(lead + (-1, item.shape[-1])) for item in payload]
    payload.append(small_rows)
    whole = [(i, 0, item.shape[-2], 0, item.shape[-1]) for i, item in enumerate(payload)]
    out_half, in_half = whole[0][2] // 2, whole[1][4] // 2
    out_chunks = [[whole[0]]]
    if out_half % 16 == 0:
        out_chunks = [[(0, at, out_half, 0, width)] for at in (0, out_half)]
    in_chunks = [[(1, 0, whole[1][2], at, in_half)] for at in (0, in_half)]
    chunks = out_chunks + in_chunks + [[whole[2], whole[3]], [whole[4], whole[5], whole[6]]]
    reduced = reduce_everywhere(fsdp, replicas, payload, chunks)
    r_w_out, r_w_in, r_q, r_k, r_v, r_w_proj = (
        item.reshape(-1, item.shape[-1]) for item in reduced[:6]
    )
    r_w_qkv = jnp.concatenate([r_q, r_k, r_v], axis=1)
    totals = reduced[6].reshape(-1, width)[:row_count].astype(f32)
    group = lax.axis_index("fsdp")

    def own(values):
        size = values.shape[-1] // fsdp
        return lax.dynamic_slice_in_dim(values, group * size, size, values.ndim - 1)

    r_small = [
        own(totals[5:7]),
        own(totals[7:9]),
        own(totals[2:5].reshape(-1)),
        own(jnp.sum(totals[0:2].reshape(2, H, HD), axis=1)),
        own(totals[9:11]),
        own(totals[11:].reshape(-1)),
    ]
    return (
        block_out.reshape(rows, slots, width),
        grad_patches,
        r_small[0],
        r_small[1],
        r_w_qkv.astype(f32),
        r_small[2],
        r_small[3],
        r_w_proj.astype(f32),
        r_small[4],
        r_w_in.astype(f32),
        r_small[5],
        r_w_out.astype(f32),
    )


def solution(mesh):
    fsdp = mesh.shape["fsdp"]
    replicas = mesh.shape["dp"]
    every = ("dp", "fsdp")
    by_row = P(every, None, None)
    last, lead = P(None, "fsdp"), P("fsdp", None)
    placed = (
        by_row,
        last,
        last,
        lead,
        P("fsdp"),
        last,
        lead,
        last,
        lead,
        P("fsdp"),
        lead,
        P(every, None),
        by_row,
    )
    outs = (by_row, by_row, last, last, lead, P("fsdp"), last, lead, last, lead, P("fsdp"), lead)
    return jax.shard_map(
        functools.partial(on_device, fsdp, replicas),
        mesh=mesh,
        in_specs=placed,
        out_specs=outs,
        check_vma=False,
    )
```
